32 devices in a mesh: grp: 1, tok: 32 (over z, y, x, core).
Axes of the slice: x: 2, y: 2, z: 4, core: 2. Of those that a mesh axis runs over, the one named last changes fastest.
Arguments:
- queries: bfloat16 [4096, 2048], P(('grp', 'tok')), may hold values from -16 to 16
- keys: bfloat16 [4096, 2048], P(('grp', 'tok')), may hold values from -16 to 16
- values: bfloat16 [4096, 2048], P(('grp', 'tok')), may hold values from -6 to 6
- segment: int32 [4096], P(('grp', 'tok')), may hold values from 0 to 41, never falling along the last dimension, each value on 1 to 256 neighbouring positions
- rates: float32 [4096, 2], P(('grp', 'tok')), may hold values from 0.00046875 to 0.0046875
- fast_one: bfloat16 [2048, 512], P(('grp', 'tok')), may hold values from -0.1875 to 0.1875
- fast_three: bfloat16 [2048, 512], P(('grp', 'tok')), may hold values from -0.1875 to 0.1875
- fast_two: bfloat16 [2048, 512], P(('grp', 'tok')), may hold values from -0.25 to 0.25
Outputs:
- attended: bfloat16 [4096, 2048], P(('grp', 'tok'))
- fast_out: bfloat16 [4096, 2048], P(('grp', 'tok'))
The draws below stay inside these ranges and needn't reach their ends.
Inputs may be any that keep to these rules, and one draw needn't show every extreme that they name: `segment`: exemplar numbers never fall along the tokens; each exemplar covers 1 to 256 consecutive tokens.
All inputs are finite; a program needn't handle non-finite values.
Results may differ from the reference program's by a relative error of at most 0.0084.
Values may be sent and summed in bfloat16 or wider, within the bound.
A program may use at most 128 MiB of HBM per device.

```python
import math
import jax
import jax.numpy as jnp
import numpy as np
from jax import lax

D = 2048
ATT_HEADS = 16
FAST_HEADS = 2
FAST_DIM = 1024
FAST_HID = 512
WINDOW = 128
TOKENS = 4096
SEGS = 42
SEG_MOST = 256


def paired_rows(key):
    base = jax.random.fold_in(key, 7)
    key_q, key_k = jax.random.split(base, 2)
    queries = jnp.clip(jax.random.normal(key_q, (TOKENS, D), jnp.float32), -6.0, 6.0)
    keys = jnp.clip(jax.random.normal(key_k, (TOKENS, D), jnp.float32), -6.0, 6.0)
    return (queries, keys)


def draw_queries(key, part):
    return paired_rows(key)[0].astype(jnp.bfloat16)


def draw_keys(key, part):
    return paired_rows(key)[1].astype(jnp.bfloat16)


def shard_levels(key, extent, shards, least, high):
    factor_of, own = 1.0, jax.random.fold_in(key, 6)
    for dim, blocks in shards:
        steps = jnp.exp(jax.random.uniform(jax.random.fold_in(own, dim), (blocks,), jnp.float32, least / len(shards), high / len(shards)))
        factor_of = factor_of * jnp.repeat(steps, extent[dim] // blocks).reshape([-1 if axis == dim else 1 for axis in range(len(extent))])
    return factor_of


def profile(amount, total, bound, skew):
    portions = [(1 << 20) // math.isqrt(standing ** skew) + 1 for standing in range(2, amount + 1)]
    rest, given = total - bound - (amount - 1), [1] * (amount - 1)
    while rest > 0:
        candidates = [i for i in range(amount - 1) if given[i] < bound]
        whole, left = sum([portions[i] for i in candidates]), rest
        for i in candidates:
            extra = min(bound - given[i], max(1, left * portions[i] // whole), rest)
            given[i] = given[i] + extra
            rest = rest - extra
    return np.array([bound] + given)


def ragged_sizes(rng, amount, total, reach, skew):
    if amount == 2:
        one = jax.random.randint(rng, (), max(1, total - reach), min(reach, total - 1) + 1)
        return jnp.stack([one, total - one])
    tallies = jnp.asarray(profile(amount, total, reach, skew), jnp.int32)
    couples = (amount - 1) // 2
    donor, taker = tallies[1:1 + 2 * couples:2], tallies[2:2 + 2 * couples:2]
    room = jnp.minimum(donor - 1, reach - taker)
    moved = jax.random.randint(jax.random.fold_in(rng, 1), (couples,), 0, 1 << 20) % (room + 1)
    tallies = tallies.at[1:1 + 2 * couples:2].set(donor - moved).at[2:2 + 2 * couples:2].set(taker + moved)
    return tallies[jax.random.permutation(jax.random.fold_in(rng, 2), amount)]


def noise(stream_key, shape, scale, reach, cuts=(), kind=jnp.bfloat16):
    entries = jax.random.normal(stream_key, shape, jnp.float32) * scale
    if len(cuts) > 0:
        entries = shard_levels(stream_key, shape, cuts, -0.22, 0.18) * entries
    return jnp.clip(entries, min=-reach, max=reach).astype(kind)


def setup_inputs(seed: int = 0, part: int = 0) -> dict:
    key_list = jax.random.split(jax.random.key(seed), 9)
    part_splits = jax.random.split(jax.random.fold_in(key_list[8], part), 9)
    queries = draw_queries(jax.random.fold_in(jax.random.fold_in(key_list[8], part), 71), part)
    keys = draw_keys(jax.random.fold_in(jax.random.fold_in(key_list[8], part), 71), part)
    values = noise(part_splits[2], (TOKENS, D), 1.0, 6.0, ((0, 32),))
    segment = jnp.searchsorted(jnp.cumsum(ragged_sizes(part_splits[3], SEGS, TOKENS, SEG_MOST, 1)), jnp.arange(TOKENS), side="right").astype(jnp.int32)
    rates = jnp.clip(jnp.exp(math.log(0.0046875) - 2.3025852 * jax.random.uniform(part_splits[4], (TOKENS, FAST_HEADS), jnp.float32) ** shard_levels(part_splits[4], (TOKENS, FAST_HEADS), ((0, 32),), -0.2, 0.2)), 0.00046875, 0.0046875)
    fast_one = noise(part_splits[5], (FAST_HEADS * FAST_DIM, FAST_HID), FAST_DIM ** -0.5, 0.1875, ((0, 32),))
    fast_three = noise(part_splits[6], (FAST_HEADS * FAST_DIM, FAST_HID), FAST_DIM ** -0.5, 0.1875, ((0, 32),))
    fast_two = noise(part_splits[7], (FAST_HEADS * FAST_DIM, FAST_HID), FAST_HID ** -0.5, 0.25, ((0, 32),))
    return dict(queries=queries, keys=keys, values=values, segment=segment, rates=rates, fast_one=fast_one, fast_three=fast_three, fast_two=fast_two)


EPS = 1e-06

def attend(queries, keys, values, segment):
    head_dim = D // ATT_HEADS
    scale = 1.0 / math.sqrt(head_dim)
    blocks = queries.shape[0] // WINDOW
    pad_keys = jnp.concatenate([jnp.zeros((WINDOW, D), keys.dtype), keys], 0)
    pad_values = jnp.concatenate([jnp.zeros((WINDOW, D), values.dtype), values], 0)
    pad_seg = jnp.concatenate([jnp.full((WINDOW,), -1, jnp.int32), segment.astype(jnp.int32)], 0)

    def one_block(index):
        start = (index * WINDOW).astype(jnp.int32)
        q_blk = lax.dynamic_slice_in_dim(queries, start, WINDOW, 0)
        k_blk = lax.dynamic_slice_in_dim(pad_keys, start, 2 * WINDOW, 0)
        v_blk = lax.dynamic_slice_in_dim(pad_values, start, 2 * WINDOW, 0)
        s_blk = lax.dynamic_slice_in_dim(pad_seg, start, 2 * WINDOW, 0)
        s_own = lax.dynamic_slice_in_dim(segment.astype(jnp.int32), start, WINDOW, 0)
        qh = q_blk.reshape(WINDOW, ATT_HEADS, head_dim).astype(jnp.float32)
        kh = k_blk.reshape(2 * WINDOW, ATT_HEADS, head_dim).astype(jnp.float32)
        vh = v_blk.reshape(2 * WINDOW, ATT_HEADS, head_dim).astype(jnp.float32)
        scores = jnp.einsum('qhd,khd->hqk', qh, kh) * scale
        rows = jnp.arange(WINDOW, dtype=jnp.int32)[:, None] + WINDOW
        cols = jnp.arange(2 * WINDOW, dtype=jnp.int32)[None, :]
        allowed = (cols <= rows) & (rows - cols < WINDOW) & (s_blk[None, :] == s_own[:, None])
        masked = jnp.where(allowed[None], scores, jnp.float32(-1e+30))
        top = lax.optimization_barrier(jnp.max(masked, axis=2, keepdims=True))
        expo = jnp.where(allowed[None], jnp.exp(masked - top), jnp.float32(0.0))
        probs = (expo / lax.optimization_barrier(jnp.sum(expo, axis=2, keepdims=True))).astype(jnp.bfloat16)
        out = jnp.einsum('hqk,khd->qhd', probs.astype(jnp.float32), vh)
        return out.reshape(WINDOW, D).astype(jnp.bfloat16)
    outs = lax.map(one_block, jnp.arange(blocks, dtype=jnp.int32))
    return outs.reshape(blocks * WINDOW, D)

def heads_apply(rows, weight):
    grouped = rows.reshape(rows.shape[0], FAST_HEADS, FAST_DIM).astype(jnp.float32)
    matrix = weight.reshape(FAST_HEADS, FAST_DIM, FAST_HID).astype(jnp.float32)
    return jnp.einsum('thd,hdc->thc', grouped, matrix)

def outer_sum(rows, hidden):
    grouped = rows.reshape(rows.shape[0], FAST_HEADS, FAST_DIM).astype(jnp.float32)
    return jnp.einsum('thd,thc->hdc', grouped, hidden.astype(jnp.float32))

def renorm(weight, grad):
    matrix = weight.reshape(FAST_HEADS, FAST_DIM, FAST_HID).astype(jnp.float32)
    update = matrix - grad
    old_len = jnp.sqrt(lax.optimization_barrier(jnp.sum(matrix * matrix, axis=1)))
    new_len = jnp.sqrt(lax.optimization_barrier(jnp.sum(update * update, axis=1)) + EPS)
    return (update * (old_len / new_len)[:, None, :]).astype(jnp.bfloat16)

def reference(queries, keys, values, segment, rates, fast_one, fast_three, fast_two):
    attended = attend(queries, keys, values, segment)
    width = FAST_HEADS * FAST_DIM
    key_fast = keys[:, :width]
    value_fast = values[:, :width]
    query_fast = queries[:, :width]
    rate = rates.astype(jnp.float32)[:, :, None]
    a_one = heads_apply(key_fast, fast_one)
    a_three = heads_apply(key_fast, fast_three)
    sig = jax.nn.sigmoid(a_one)
    weighted = (-rate * a_one * sig * a_three).astype(jnp.bfloat16)
    grad_two = outer_sum(value_fast, weighted)
    back = -rate * heads_apply(value_fast, fast_two)
    delta_one = (back * a_three * sig * (1.0 + a_one * (1.0 - sig))).astype(jnp.bfloat16)
    delta_three = (back * a_one * sig).astype(jnp.bfloat16)
    grad_one = outer_sum(key_fast, delta_one)
    grad_three = outer_sum(key_fast, delta_three)
    new_one = renorm(fast_one, grad_one)
    new_three = renorm(fast_three, grad_three)
    new_two = renorm(fast_two, grad_two)
    grouped = query_fast.reshape(query_fast.shape[0], FAST_HEADS, FAST_DIM).astype(jnp.float32)
    b_one = jnp.einsum('thd,hdc->thc', grouped, new_one.astype(jnp.float32))
    b_three = jnp.einsum('thd,hdc->thc', grouped, new_three.astype(jnp.float32))
    mixed = (jax.nn.silu(b_one) * b_three).astype(jnp.bfloat16)
    fast_out = jnp.einsum('thc,hdc->thd', mixed.astype(jnp.float32), new_two.astype(jnp.float32))
    fast_out = fast_out.reshape(query_fast.shape[0], width).astype(jnp.bfloat16)
    return (attended, fast_out)
```

```python
import functools
import math

import jax
import jax.numpy as jnp
from jax import lax
from jax.experimental import pallas as pl
from jax.experimental.pallas import tpu as pltpu
from jax.sharding import PartitionSpec as P

ATT_HEADS = 16
FAST_HEADS = 2
WINDOW = 128
EPS = 1e-06

ONE, THREE, TWO = 0, 1, 2


def device(line, x, y, core):
    return ((line * 2 + y) * 2 + x) * 2 + core


def in_role(line, a, b, role):
    return device(line, a + role * (b - a), b + role * (a - b), role)


def bit_of(index, bit):
    return lax.rem(lax.div(index, jnp.int32(1 << bit)), jnp.int32(2))


def flipped(index, bit):
    return index + (1 - 2 * bit_of(index, bit)) * (1 << bit)


def remote(src, dst, send_sem, recv_sem, partner):
    return pltpu.make_async_remote_copy(
        src_ref=src,
        dst_ref=dst,
        send_sem=send_sem,
        recv_sem=recv_sem,
        device_id={"tok": partner},
        device_id_type=pl.DeviceIdType.MESH,
    )


def turned(row, size):
    return jnp.transpose(jnp.broadcast_to(row, (size, size)))


def nt_dot(left, right):
    return lax.dot_general(
        left, right, (((1,), (1,)), ((), ())), preferred_element_type=jnp.float32
    )


def dot(left, right):
    return jnp.dot(left, right, preferred_element_type=jnp.float32)


def flat(blocks):
    n, unit, width = blocks.shape
    if unit % 16 == 0:
        return blocks.reshape(n * unit, width)
    return blocks.astype(jnp.float32).reshape(n * unit, width).astype(jnp.bfloat16)


def kernel(count, *refs):
    w_refs = refs[:3]
    q_ref, k_ref, v_ref, seg_ref, rate_ref = refs[3:8]
    att_ref, out_ref = refs[8:10]
    (
        wbuf, kbuf, vbuf, qbuf, rbuf, rsend, asum, hid, total, staged, landed, old_own, old_all, new,
        z_own, z_peer, z_send, o_send, old_k, old_v, old_seg,
        first_s, first_r, first_l, mirror_s, mirror_r, mate_s, mate_r, side_s, side_r,
        tok_s, tok_r, sum_s, sum_r, all_s, all_r, end_s, end_r, halo_s, halo_r,
    ) = refs[10:]

    lines = count // 8
    half = lines // 2
    line_bits = lines.bit_length() - 1
    steps = line_bits + 1
    rows, hidden = w_refs[0].shape
    cols = hidden // 2
    tokens, width = q_ref.shape
    feats = width // FAST_HEADS
    blocks = 2 * lines
    unit = cols // blocks

    me = lax.axis_index("tok")
    core, chip = lax.rem(me, 2), lax.div(me, 2)
    x, y, line = lax.rem(chip, 2), lax.rem(lax.div(chip, 2), 2), lax.div(chip, 4)
    a, b = x + core * (y - x), y + core * (x - y)
    a_other, b_other = b, a
    other = 1 - core
    partner = device(line, x, y, other)
    pair = in_role(line, 1 - a, b, core)
    side = in_role(line, a, 1 - b, core)
    pair_sends = pair + other - core
    pair_takes = in_role(line, 1 - a_other, b_other, other)
    mirror_line = lax.rem(line + half, lines)
    mirror = in_role(mirror_line, a, b, core)
    upper = lax.div(line, half)
    place = line - upper * half
    base = upper * half

    def mate(i):
        return in_role(base + lax.rem(place + i, half), a, b, core)

    after, before = lax.rem(me + 1, count), lax.rem(me + count - 1, count)

    for group in range(FAST_HEADS):
        column = jnp.broadcast_to(rate_ref[:, group : group + 1], (tokens, tokens))
        rsend[group] = jnp.transpose(column)[0:8, :]

    barrier = pltpu.get_barrier_semaphore()
    known = [partner, pair, side, pair_sends, pair_takes, mirror, after, before]
    known += [mate(i) for i in range(1, half)]
    for one in known:
        pl.semaphore_signal(
            barrier, inc=1, device_id={"tok": one}, device_id_type=pl.DeviceIdType.MESH
        )
    pl.semaphore_wait(barrier, len(known))

    started = []

    def go(copy):
        copy.start()
        started.append(copy)

    head = upper
    head_a, head_b = x + head * (y - x), y + head * (x - y)
    stored = place * 4 + y * 2 + x

    def first(m, copy_half, kind):
        lanes = pl.ds(pl.multiple_of(copy_half * cols, cols), cols)
        src = w_refs[m].at[:, lanes]
        dst = wbuf.at[m, stored, pl.ds(pl.multiple_of(core * rows, rows), rows), :]
        if kind == "here":
            return pltpu.make_async_copy(src, dst, first_l.at[m])
        if kind == "core":
            return remote(src, dst, first_s.at[m, 0], first_r.at[m, 0], device(line, x, y, head))
        to = in_role(line, 1 - head_a, head_b, head)
        return remote(src, dst, first_s.at[m, 1], first_r.at[m, 1 + core], to)

    for m in range(3):
        go(first(m, 1 - head_a, "pair"))

        @pl.when(core == head)
        def _():
            first(m, head_a, "here").start()

        @pl.when(core != head)
        def _():
            first(m, head_a, "core").start()

    def own_lanes(group):
        return pl.ds(pl.multiple_of(group * feats, feats), feats)

    def send_tokens(kind):
        ref, buf = ((k_ref, kbuf), (v_ref, vbuf), (q_ref, qbuf), (rsend, rbuf))[kind]
        if kind == 3:
            mine, theirs = ref.at[core], ref.at[other]
        else:
            mine, theirs = ref.at[:, own_lanes(core)], ref.at[:, own_lanes(other)]
        here, there = buf.at[a * 2 + core], buf.at[a_other * 2 + core]
        go(remote(mine, here, tok_s.at[kind, 0], tok_r.at[kind, 1 + core], pair))
        go(remote(theirs, there, tok_s.at[kind, 1], tok_r.at[kind, 0], partner))
        go(remote(theirs, there, tok_s.at[kind, 2], tok_r.at[kind, 1 + core], pair_takes))
        if kind == 3:
            rbuf[a * 2 + core] = rsend[core]
        else:
            buf[a * 2 + core] = ref[:, own_lanes(core)]

    def take_tokens(kind):
        buf = (kbuf, vbuf, qbuf, rbuf)[kind]
        for i, slot in ((0, a * 2 + other), (1, (1 - a) * 2), (2, (1 - a) * 2 + 1)):
            ref = buf.at[slot]
            remote(ref, ref, tok_s.at[kind, i], tok_r.at[kind, i], partner).wait_recv()

    send_tokens(0)
    send_tokens(3)
    send_tokens(1)

    def piece(m, k, a_from, b_from):
        return wbuf.at[m, k * 4 + b_from * 2 + a_from + core * (a_from - b_from)]

    def first_wait(m):
        def part(a_from, c):
            ref = wbuf.at[m, place * 4 + b * 2 + a_from + core * (a_from - b)]
            return ref.at[pl.ds(pl.multiple_of(c * rows, rows), rows), :]

        first(m, head_a, "here").wait()
        ref = part(a, other)
        remote(ref, ref, first_s.at[m, 0], first_r.at[m, 0], partner).wait_recv()
        for c in range(2):
            ref = part(1 - a, c)
            remote(ref, ref, first_s.at[m, 1], first_r.at[m, 1 + c], pair).wait_recv()

    def to_mirror(m, i):
        ref = piece(m, place, i, b)
        return remote(ref, ref, mirror_s.at[m, i], mirror_r.at[m, i], mirror)

    def to_mate(m, i, step):
        ref = piece(m, place, i, b)
        return remote(ref, ref, mate_s.at[m, i, step], mate_r.at[m, i, step], mate(step))

    def from_mate(m, i, step):
        ref = piece(m, lax.rem(place + half - step, half), i, b)
        return remote(ref, ref, mate_s.at[m, i, step], mate_r.at[m, i, step], mate(step))

    def to_side(m, i, step):
        ref = piece(m, lax.rem(place + half - step, half), i, b)
        return remote(ref, ref, side_s.at[m, i, step], side_r.at[m, i, step], side)

    def from_side(m, i, step):
        ref = piece(m, lax.rem(place + half - step, half), i, 1 - b)
        return remote(ref, ref, side_s.at[m, i, step], side_r.at[m, i, step], side)

    for m in range(3):

        @pl.when(core == head)
        def _():
            first_wait(m)
            for i in range(2):
                to_mirror(m, i).start()

        @pl.when(core != head)
        def _():
            for i in range(2):
                to_mirror(m, i).wait_recv()

        for i in range(2):
            for step in range(1, half):
                go(to_mate(m, i, step))
            go(to_side(m, i, 0))
    for m in range(3):
        for step in range(1, half):
            for i in range(2):
                from_mate(m, i, step).wait_recv()
                go(to_side(m, i, step))

    def weight_there(m):
        for step in range(half):
            for i in range(2):
                from_side(m, i, step).wait_recv()

    def weight(m):
        return wbuf[m].reshape(feats, cols)

    all_keys = lambda: kbuf[...].reshape(4 * tokens, feats)
    all_values = lambda: vbuf[...].reshape(4 * tokens, feats)

    take_tokens(0)
    take_tokens(3)
    for m in (ONE, THREE):
        weight_there(m)
        asum[m] = dot(all_keys(), weight(m)).reshape(4, tokens, cols)

    def spread(s):
        column = turned(rbuf[s][0:1, :], tokens)
        return jnp.concatenate([column] * (cols // tokens), axis=1)

    def keep(m, s, value):
        lanes = pl.ds(pl.multiple_of(s * tokens, tokens), tokens)
        hid[m, :, lanes] = jnp.transpose(value).astype(jnp.bfloat16)

    def weigh(s, carry):
        a_one, a_three = asum[ONE, s], asum[THREE, s]
        keep(TWO, s, -spread(s) * a_one * jax.nn.sigmoid(a_one) * a_three)
        return carry

    lax.fori_loop(0, 4, weigh, 0)
    take_tokens(1)

    line_bit = [bit_of(line, i) for i in range(line_bits)]
    starts = [jnp.int32(0)]
    for i in range(line_bits):
        starts.append(starts[-1] + line_bit[i] * (lines >> (i + 1)))
    pos = b * lines + starts[-1]

    def gradient(m, which):
        at = pl.ds(pl.multiple_of(which * (cols // 2), cols // 2), cols // 2)
        grad = dot(hid[m, at, :], all_values() if m == TWO else all_keys())
        return grad.reshape(lines, unit, feats)

    def offset(step):
        return blocks - 2 * (lines >> step)

    def send_sum(m, step):
        at = pl.ds(offset(step), lines >> step)
        to = side if step == 0 else in_role(flipped(line, step - 1), a, b, core)
        return remote(
            staged.at[m, at], landed.at[m, at], sum_s.at[m, step], sum_r.at[m, step], to
        )

    def send_away(m):
        staged[m, pl.ds(0, lines)] = gradient(m, 1 - b).astype(jnp.bfloat16)
        go(send_sum(m, 0))

    def keep_own(m):
        total[m] = gradient(m, b)

    send_away(TWO)
    weight_there(TWO)
    asum[TWO] = dot(all_values(), weight(TWO)).reshape(4, tokens, cols)

    def deltas(s, carry):
        a_one, a_three = asum[ONE, s], asum[THREE, s]
        back = -spread(s) * asum[TWO, s]
        sig = jax.nn.sigmoid(a_one)
        keep(ONE, s, back * a_three * sig * (1.0 + a_one * (1.0 - sig)))
        keep(THREE, s, back * a_one * sig)
        return carry

    lax.fori_loop(0, 4, deltas, 0)
    send_away(ONE)
    send_away(THREE)
    send_tokens(2)
    halo = [
        remote(src, dst, halo_s.at[i], halo_r.at[i], after)
        for i, (src, dst) in enumerate(((seg_ref, old_seg), (k_ref, old_k), (v_ref, old_v)))
    ]

    @pl.when(me != count - 1)
    def _():
        for copy in halo:
            copy.start()

    @pl.when(me == 0)
    def _():
        old_k[...] = jnp.zeros_like(old_k)
        old_v[...] = jnp.zeros_like(old_v)
        old_seg[...] = jnp.zeros_like(old_seg)

    order = (TWO, ONE, THREE)
    for m in order:
        keep_own(m)
    for m in order:
        lanes = pl.ds(pl.multiple_of(b * (cols // 2), cols // 2), cols // 2)
        mine = wbuf[m, :, :, lanes].reshape(feats, cols // 2).astype(jnp.float32)
        old_all[...] = jnp.transpose(mine).reshape(lines, unit, feats)
        old_own[m] = old_all[starts[-1]]
    for step in range(1, steps):
        size = lines >> step
        bit = line_bit[step - 1]
        kept, away = starts[step], starts[step - 1] + (1 - bit) * size
        shift = offset(step - 1) - starts[step - 1]
        for m in order:
            send_sum(m, step - 1).wait_recv()

            def stage(i, carry):
                value = total[m, away + i] + landed[m, shift + away + i].astype(jnp.float32)
                staged[m, offset(step) + i] = value.astype(jnp.bfloat16)
                return carry

            def hold(i, carry):
                value = total[m, kept + i] + landed[m, shift + kept + i].astype(jnp.float32)
                total[m, kept + i] = value
                return carry

            lax.fori_loop(0, size, stage, 0)
            go(send_sum(m, step))
            lax.fori_loop(0, size, hold, 0)

    def span(part, position):
        if part == 0:
            return pl.ds(position, 1)
        size = 1 << (part - 1)
        return pl.ds(flipped(lax.div(position, jnp.int32(size)), 0) * size, size)

    def send_new(m, step, part):
        src = new.at[m, 0, span(part, pos)]
        if step == steps:
            dst, to = new.at[m, 1, span(part, pos)], pair
        elif step == steps - 1:
            dst, to = src, side
        else:
            dst, to = src, in_role(flipped(line, line_bits - 1 - step), a, b, core)
        return remote(src, dst, all_s.at[m, step, part], all_r.at[m, step, part], to)

    def new_there(m, step, part):
        if step == steps:
            ref = new.at[m, 1, span(part, pos)]
        else:
            ref = new.at[m, 0, span(part, flipped(pos, step))]
        return remote(ref, ref, all_s.at[m, step, part], all_r.at[m, step, part], side)

    def last_step(m):
        return steps + 1 if m == TWO else steps

    for m in order:
        send_sum(m, steps - 1).wait_recv()
        grad = total[m, starts[-1]] + landed[m, offset(steps - 1)].astype(jnp.float32)
        old = old_own[m]
        update = old - grad
        old_len = jnp.sqrt(jnp.sum(old * old, axis=1, keepdims=True))
        new_len = jnp.sqrt(jnp.sum(update * update, axis=1, keepdims=True) + EPS)
        new[m, 0, pos] = (update * (old_len / new_len)).astype(jnp.bfloat16)
        for step in range(last_step(m)):
            go(send_new(m, step, 0))

    dim = width // ATT_HEADS
    scale = 1.0 / math.sqrt(dim)

    @pl.when(me != 0)
    def _():
        for copy in halo:
            copy.wait_recv()

    def attend(first_head, last_head):
        row = lax.broadcasted_iota(jnp.int32, (tokens, tokens), 0)
        col = lax.broadcasted_iota(jnp.int32, (tokens, tokens), 1)
        seg_row = seg_ref[...].astype(jnp.float32)
        seg_col = turned(seg_row, tokens)
        now_ok = (col <= row) & (row - col < WINDOW) & (seg_col == seg_row)
        old_ok = (
            (row - col + tokens < WINDOW)
            & (seg_col == old_seg[...].astype(jnp.float32))
            & (row + me * tokens >= row + tokens)
        )

        def one(i, carry):
            lanes = pl.ds(pl.multiple_of(i * dim, dim), dim)
            q = q_ref[:, lanes]

            def score(keys, allowed):
                return jnp.where(allowed, nt_dot(q, keys) * scale, jnp.float32(-1e30))

            old, now = score(old_k[:, lanes], old_ok), score(k_ref[:, lanes], now_ok)
            top = jnp.maximum(
                jnp.max(old, axis=1, keepdims=True), jnp.max(now, axis=1, keepdims=True)
            )
            old = jnp.where(old_ok, jnp.exp(old - top), jnp.float32(0.0))
            now = jnp.where(now_ok, jnp.exp(now - top), jnp.float32(0.0))
            norm = jnp.sum(old, axis=1, keepdims=True) + jnp.sum(now, axis=1, keepdims=True)
            out = dot((old / norm).astype(jnp.bfloat16), old_v[:, lanes]) + dot(
                (now / norm).astype(jnp.bfloat16), v_ref[:, lanes]
            )
            att_ref[:, lanes] = out.astype(jnp.bfloat16)
            return carry

        lax.fori_loop(first_head, last_head, one, 0)

    for step in range(steps):
        for m in order:
            for part in range(step + 1):
                new_there(m, step, part).wait_recv()
            for later in range(step + 1, last_step(m)):
                go(send_new(m, later, step + 1))
        attend(ATT_HEADS * step // steps, ATT_HEADS * (step + 1) // steps)

    take_tokens(2)

    def mixed(place_from):
        rows_q = qbuf[pl.ds(place_from * 2, 2)].reshape(2 * tokens, feats)
        b_one = nt_dot(rows_q, flat(new[ONE, 0]))
        b_three = nt_dot(rows_q, flat(new[THREE, 0]))
        return (jax.nn.silu(b_one) * b_three).astype(jnp.bfloat16)

    z_send[...] = mixed(1 - a)
    z_copy = remote(z_send, z_peer, end_s.at[0], end_r.at[0], pair)
    go(z_copy)
    z_own[...] = mixed(a)
    for part in range(steps + 1):
        new_there(TWO, steps, part).wait_recv()
    z_copy.wait_recv()

    def fast_rows(c):
        at = pl.ds(pl.multiple_of(c * tokens, tokens), tokens)
        value = dot(z_own[at, :], flat(new[TWO, 0])) + dot(z_peer[at, :], flat(new[TWO, 1]))
        return value.astype(jnp.bfloat16)

    o_send[...] = fast_rows(other)
    out_copy = remote(
        o_send, out_ref.at[:, own_lanes(core)], end_s.at[1], end_r.at[1], partner
    )
    go(out_copy)
    out_ref[:, own_lanes(core)] = fast_rows(core)
    theirs = out_ref.at[:, own_lanes(other)]
    remote(theirs, theirs, end_s.at[1], end_r.at[1], partner).wait_recv()

    for copy in started:
        copy.wait_send()
    for m in range(3):

        @pl.when(core == head)
        def _():
            for i in range(2):
                to_mirror(m, i).wait_send()

        @pl.when(core != head)
        def _():
            first(m, head_a, "core").wait_send()

    @pl.when(me != count - 1)
    def _():
        for copy in halo:
            copy.wait_send()


def per_device(queries, keys, values, segment, rates, fast_one, fast_three, fast_two):
    count = lax.axis_size("tok")
    tokens, width = queries.shape
    rows, hidden = fast_one.shape
    lines = count // 8
    half = lines // 2
    steps = lines.bit_length()
    feats = width // FAST_HEADS
    cols = hidden // 2
    blocks = 2 * lines
    unit = cols // blocks
    bf16, f32 = jnp.bfloat16, jnp.float32
    dma = pltpu.SemaphoreType.DMA
    return pl.pallas_call(
        functools.partial(kernel, count),
        out_shape=[jax.ShapeDtypeStruct(queries.shape, bf16)] * 2,
        in_specs=[pl.BlockSpec(memory_space=pltpu.VMEM)] * 8,
        out_specs=[pl.BlockSpec(memory_space=pltpu.VMEM)] * 2,
        scratch_shapes=[
            pltpu.VMEM((3, count // 4, 2 * rows, cols), bf16),
            pltpu.VMEM((4, tokens, feats), bf16),
            pltpu.VMEM((4, tokens, feats), bf16),
            pltpu.VMEM((4, tokens, feats), bf16),
            pltpu.VMEM((4, 8, tokens), f32),
            pltpu.VMEM((FAST_HEADS, 8, tokens), f32),
            pltpu.VMEM((3, 4, tokens, cols), f32),
            pltpu.VMEM((3, cols, 4 * tokens), bf16),
            pltpu.VMEM((3, lines, unit, feats), f32),
            pltpu.VMEM((3, blocks, unit, feats), bf16),
            pltpu.VMEM((3, blocks, unit, feats), bf16),
            pltpu.VMEM((3, unit, feats), f32),
            pltpu.VMEM((lines, unit, feats), f32),
            pltpu.VMEM((3, 2, blocks, unit, feats), bf16),
            pltpu.VMEM((2 * tokens, cols), bf16),
            pltpu.VMEM((2 * tokens, cols), bf16),
            pltpu.VMEM((2 * tokens, cols), bf16),
            pltpu.VMEM((tokens, feats), bf16),
            pltpu.VMEM(keys.shape, bf16),
            pltpu.VMEM(values.shape, bf16),
            pltpu.VMEM((1, tokens), jnp.int32),
            dma((3, 2)),
            dma((3, 3)),
            dma((3,)),
            dma((3, 2)),
            dma((3, 2)),
            dma((3, 2, half)),
            dma((3, 2, half)),
            dma((3, 2, half)),
            dma((3, 2, half)),
            dma((4, 3)),
            dma((4, 3)),
            dma((3, steps)),
            dma((3, steps)),
            dma((3, steps + 1, steps + 1)),
            dma((3, steps + 1, steps + 1)),
            dma((2,)),
            dma((2,)),
            dma((3,)),
            dma((3,)),
        ],
        compiler_params=pltpu.CompilerParams(collective_id=0, has_side_effects=True),
    )(
        fast_one, fast_three, fast_two, queries, keys, values, segment.reshape(1, tokens), rates
    )


def solution(mesh):
    placed = P(("grp", "tok"), None)
    return jax.shard_map(
        per_device,
        mesh=mesh,
        in_specs=(placed, placed, placed, P(("grp", "tok")), placed, placed, placed, placed),
        out_specs=(placed, placed),
        check_vma=False,
    )
```

```python
import functools
import math

import jax
import jax.numpy as jnp
from jax import lax
from jax.experimental import pallas as pl
from jax.experimental.pallas import tpu as pltpu
from jax.sharding import PartitionSpec as P

ATT_HEADS = 16
FAST_HEADS = 2
WINDOW = 128
EPS = 1e-06

ONE, THREE, TWO = 0, 1, 2
WIDE = ()


def device(line, x, y, core):
    return ((line * 2 + y) * 2 + x) * 2 + core


def in_role(line, a, b, role):
    return device(line, a + role * (b - a), b + role * (a - b), role)


def bit_of(index, bit):
    return lax.rem(lax.div(index, jnp.int32(1 << bit)), jnp.int32(2))


def flipped(index, bit):
    return index + (1 - 2 * bit_of(index, bit)) * (1 << bit)


def remote(src, dst, send_sem, recv_sem, partner):
    return pltpu.make_async_remote_copy(
        src_ref=src,
        dst_ref=dst,
        send_sem=send_sem,
        recv_sem=recv_sem,
        device_id={"tok": partner},
        device_id_type=pl.DeviceIdType.MESH,
    )


def turned(row, size):
    return jnp.transpose(jnp.broadcast_to(row, (size, size)))


def nt_dot(left, right):
    return lax.dot_general(
        left, right, (((1,), (1,)), ((), ())), preferred_element_type=jnp.float32
    )


def dot(left, right):
    return jnp.dot(left, right, preferred_element_type=jnp.float32)


def flat(blocks):
    n, unit, width = blocks.shape
    if unit % 16 == 0:
        return blocks.reshape(n * unit, width)
    return blocks.astype(jnp.float32).reshape(n * unit, width).astype(jnp.bfloat16)


def kernel(count, *refs):
    w_refs = refs[:3]
    q_ref, k_ref, v_ref, seg_ref, rate_ref = refs[3:8]
    att_ref, out_ref = refs[8:10]
    (
        wbuf, kbuf, vbuf, qbuf, rbuf, rsend, asum, hid, total, staged, landed, old_own, old_all, new,
        z_own, z_peer, z_send, o_send, old_k, old_v, old_seg,
        first_s, first_r, first_l, mirror_s, mirror_r, mate_s, mate_r, side_s, side_r,
        tok_s, tok_r, sum_s, sum_r, all_s, all_r, end_s, end_r, halo_s, halo_r,
    ) = refs[10:]

    lines = count // 8
    half = lines // 2
    line_bits = lines.bit_length() - 1
    steps = line_bits + 1
    rows, hidden = w_refs[0].shape
    cols = hidden // 2
    tokens, width = q_ref.shape
    feats = width // FAST_HEADS
    blocks = 2 * lines
    unit = cols // blocks

    me = lax.axis_index("tok")
    core, chip = lax.rem(me, 2), lax.div(me, 2)
    x, y, line = lax.rem(chip, 2), lax.rem(lax.div(chip, 2), 2), lax.div(chip, 4)
    a, b = x + core * (y - x), y + core * (x - y)
    a_other, b_other = b, a
    other = 1 - core
    partner = device(line, x, y, other)
    pair = in_role(line, 1 - a, b, core)
    side = in_role(line, a, 1 - b, core)
    pair_takes = in_role(line, 1 - a_other, b_other, other)
    mirror_line = lax.rem(line + half, lines)
    mirror = in_role(mirror_line, a, b, core)
    upper = lax.div(line, half)
    place = line - upper * half
    base = upper * half

    def mate(i):
        return in_role(base + lax.rem(place + i, half), a, b, core)

    after, before = lax.rem(me + 1, count), lax.rem(me + count - 1, count)

    for group in range(FAST_HEADS):
        rsend[group] = jnp.broadcast_to(rate_ref[group : group + 1, :], (8, tokens))

    barrier = pltpu.get_barrier_semaphore()
    plane = line * 8
    known = [plane + lax.rem(me - plane + i, 8) for i in range(1, 8)]
    known += [mirror, after, before] + [mate(i) for i in range(1, half)]
    for one in known:
        pl.semaphore_signal(
            barrier, inc=1, device_id={"tok": one}, device_id_type=pl.DeviceIdType.MESH
        )
    pl.semaphore_wait(barrier, len(known))

    started = []

    def go(copy):
        copy.start()
        started.append(copy)

    head = upper
    head_a, head_b = x + head * (y - x), y + head * (x - y)
    stored = place * 4 + y * 2 + x

    def first(m, far):
        cross, apart = far % 2, far // 2
        start = (head_a + cross - 2 * cross * head_a) * cols
        src = w_refs[m].at[:, pl.ds(pl.multiple_of(start, cols), cols)]
        dst = wbuf.at[m, stored, pl.ds(pl.multiple_of(core * rows, rows), rows), :]
        to_a = 1 - head_a if cross else head_a
        to = in_role(line, to_a, 1 - head_b if apart else head_b, head)
        return remote(src, dst, first_s.at[m, far], first_r.at[m, far, core], to)

    def first_here(m):
        src = w_refs[m].at[:, pl.ds(pl.multiple_of(head_a * cols, cols), cols)]
        dst = wbuf.at[m, stored, pl.ds(pl.multiple_of(core * rows, rows), rows), :]
        return pltpu.make_async_copy(src, dst, first_l.at[m])

    def reach(m):
        return 4 if m in WIDE else 2

    for m in range(3):
        for far in range(1, reach(m)):
            go(first(m, far))

        @pl.when(core == head)
        def _():
            first_here(m).start()

        @pl.when(core != head)
        def _():
            first(m, 0).start()

    def own_lanes(group):
        return pl.ds(pl.multiple_of(group * feats, feats), feats)

    def send_tokens(kind):
        ref, buf = ((k_ref, kbuf), (v_ref, vbuf), (q_ref, qbuf), (rsend, rbuf))[kind]
        if kind == 3:
            mine, theirs = ref.at[core], ref.at[other]
        else:
            mine, theirs = ref.at[:, own_lanes(core)], ref.at[:, own_lanes(other)]
        here, there = buf.at[a * 2 + core], buf.at[a_other * 2 + core]
        go(remote(mine, here, tok_s.at[kind, 0], tok_r.at[kind, 1 + core], pair))
        go(remote(theirs, there, tok_s.at[kind, 1], tok_r.at[kind, 0], partner))
        go(remote(theirs, there, tok_s.at[kind, 2], tok_r.at[kind, 1 + core], pair_takes))
        if kind == 3:
            rbuf[a * 2 + core] = rsend[core]
        else:
            buf[a * 2 + core] = ref[:, own_lanes(core)]

    def take_tokens(kind):
        buf = (kbuf, vbuf, qbuf, rbuf)[kind]
        for i, slot in ((0, a * 2 + other), (1, (1 - a) * 2), (2, (1 - a) * 2 + 1)):
            ref = buf.at[slot]
            remote(ref, ref, tok_s.at[kind, i], tok_r.at[kind, i], partner).wait_recv()

    send_tokens(0)
    send_tokens(3)
    send_tokens(1)

    def pairs(m):
        return 1 if m in WIDE else 2

    def piece(m, k, i, b_from):
        if m in WIDE:
            return wbuf.at[m, pl.ds(k * 4, 4)]
        return wbuf.at[m, k * 4 + b_from * 2 + i + core * (i - b_from)]

    def first_wait(m):
        first_here(m).wait()
        for far in range(reach(m)):
            from_a = 1 - a if far % 2 else a
            from_b = 1 - b if far // 2 else b
            block = wbuf.at[m, place * 4 + from_b * 2 + from_a + core * (from_a - from_b)]
            for c in (other,) if far == 0 else (0, 1):
                ref = block.at[pl.ds(pl.multiple_of(c * rows, rows), rows), :]
                copy = remote(ref, ref, first_s.at[m, far], first_r.at[m, far, c], partner)
                copy.wait_recv()

    def to_mirror(m, i):
        ref = piece(m, place, i, b)
        return remote(ref, ref, mirror_s.at[m, i], mirror_r.at[m, i], mirror)

    def to_mate(m, i, step):
        ref = piece(m, place, i, b)
        return remote(ref, ref, mate_s.at[m, i, step], mate_r.at[m, i, step], mate(step))

    def from_mate(m, i, step):
        ref = piece(m, lax.rem(place + half - step, half), i, b)
        return remote(ref, ref, mate_s.at[m, i, step], mate_r.at[m, i, step], mate(step))

    def to_side(m, i, step):
        ref = piece(m, lax.rem(place + half - step, half), i, b)
        return remote(ref, ref, side_s.at[m, i, step], side_r.at[m, i, step], side)

    def from_side(m, i, step):
        ref = piece(m, lax.rem(place + half - step, half), i, 1 - b)
        return remote(ref, ref, side_s.at[m, i, step], side_r.at[m, i, step], side)

    for m in range(3):

        @pl.when(core == head)
        def _():
            first_wait(m)
            for i in range(pairs(m)):
                to_mirror(m, i).start()

        @pl.when(core != head)
        def _():
            for i in range(pairs(m)):
                to_mirror(m, i).wait_recv()

        for i in range(pairs(m)):
            for step in range(1, half):
                go(to_mate(m, i, step))
            if m not in WIDE:
                go(to_side(m, i, 0))
    for m in range(3):
        if m in WIDE:
            continue
        for step in range(1, half):
            for i in range(2):
                from_mate(m, i, step).wait_recv()
                go(to_side(m, i, step))

    def weight_there(m):
        if m in WIDE:
            for step in range(1, half):
                from_mate(m, 0, step).wait_recv()
            return
        for step in range(half):
            for i in range(2):
                from_side(m, i, step).wait_recv()

    def weight(m):
        return wbuf[m].reshape(feats, cols)

    all_keys = lambda: kbuf[...].reshape(4 * tokens, feats)
    all_values = lambda: vbuf[...].reshape(4 * tokens, feats)

    def spread(s):
        column = turned(rbuf[s][0:1, :], tokens)
        return jnp.concatenate([column] * (cols // tokens), axis=1)

    def keep(m, s, value):
        lanes = pl.ds(pl.multiple_of(s * tokens, tokens), tokens)
        hid[m, :, lanes] = jnp.transpose(value).astype(jnp.bfloat16)

    def weigh(s, carry):
        a_one, a_three = asum[ONE, s], asum[THREE, s]
        keep(TWO, s, -spread(s) * a_one * jax.nn.sigmoid(a_one) * a_three)
        return carry

    line_bit = [bit_of(line, i) for i in range(line_bits)]
    starts = [jnp.int32(0)]
    for i in range(line_bits):
        starts.append(starts[-1] + line_bit[i] * (lines >> (i + 1)))
    pos = b * lines + starts[-1]

    def gradient(m, which):
        at = pl.ds(pl.multiple_of(which * (cols // 2), cols // 2), cols // 2)
        grad = dot(hid[m, at, :], all_values() if m == TWO else all_keys())
        return grad.reshape(lines, unit, feats)

    def offset(step):
        return blocks - 2 * (lines >> step)

    def send_sum(m, step):
        at = pl.ds(offset(step), lines >> step)
        to = side if step == 0 else in_role(flipped(line, step - 1), a, b, core)
        return remote(
            staged.at[m, at], landed.at[m, at], sum_s.at[m, step], sum_r.at[m, step], to
        )

    def send_away(m):
        staged[m, pl.ds(0, lines)] = gradient(m, 1 - b).astype(jnp.bfloat16)
        go(send_sum(m, 0))

    def keep_own(m):
        total[m] = gradient(m, b)

    def keep_old(m):
        lanes = pl.ds(pl.multiple_of(b * (cols // 2), cols // 2), cols // 2)
        mine = wbuf[m, :, :, lanes].reshape(feats, cols // 2).astype(jnp.float32)
        old_all[...] = jnp.transpose(mine).reshape(lines, unit, feats)
        old_own[m] = old_all[starts[-1]]

    def deltas(s, carry):
        a_one, a_three = asum[ONE, s], asum[THREE, s]
        back = -spread(s) * asum[TWO, s]
        sig = jax.nn.sigmoid(a_one)
        keep(ONE, s, back * a_three * sig * (1.0 + a_one * (1.0 - sig)))
        keep(THREE, s, back * a_one * sig)
        return carry

    def project(m):
        weight_there(m)
        rows_in = all_values() if m == TWO else all_keys()
        asum[m] = dot(rows_in, weight(m)).reshape(4, tokens, cols)

    take_tokens(0)
    take_tokens(3)
    project(ONE)
    project(THREE)
    lax.fori_loop(0, 4, weigh, 0)
    take_tokens(1)
    send_away(TWO)
    keep_own(TWO)
    keep_old(ONE)
    keep_old(THREE)
    project(TWO)
    lax.fori_loop(0, 4, deltas, 0)
    send_away(ONE)
    send_away(THREE)
    send_tokens(2)
    halo = [
        remote(src, dst, halo_s.at[i], halo_r.at[i], after)
        for i, (src, dst) in enumerate(((seg_ref, old_seg), (k_ref, old_k), (v_ref, old_v)))
    ]

    @pl.when(me != count - 1)
    def _():
        for copy in halo:
            copy.start()

    @pl.when(me == 0)
    def _():
        old_k[...] = jnp.zeros_like(old_k)
        old_v[...] = jnp.zeros_like(old_v)
        old_seg[...] = jnp.zeros_like(old_seg)

    order = (TWO, ONE, THREE)

    def pass_on(m, step):
        size = lines >> step
        bit = line_bit[step - 1]
        kept, away = starts[step], starts[step - 1] + (1 - bit) * size
        shift = offset(step - 1) - starts[step - 1]
        send_sum(m, step - 1).wait_recv()

        def stage(i, carry):
            value = total[m, away + i] + landed[m, shift + away + i].astype(jnp.float32)
            staged[m, offset(step) + i] = value.astype(jnp.bfloat16)
            return carry

        def hold(i, carry):
            value = total[m, kept + i] + landed[m, shift + kept + i].astype(jnp.float32)
            total[m, kept + i] = value
            return carry

        lax.fori_loop(0, size, stage, 0)
        go(send_sum(m, step))
        lax.fori_loop(0, size, hold, 0)

    def span(part, position):
        if part == 0:
            return pl.ds(position, 1)
        size = 1 << (part - 1)
        return pl.ds(flipped(lax.div(position, jnp.int32(size)), 0) * size, size)

    def send_new(m, step, part):
        src = new.at[m, 0, span(part, pos)]
        if step == steps:
            dst, to = new.at[m, 1, span(part, pos)], pair
        elif step == steps - 1:
            dst, to = src, side
        else:
            dst, to = src, in_role(flipped(line, line_bits - 1 - step), a, b, core)
        return remote(src, dst, all_s.at[m, step, part], all_r.at[m, step, part], to)

    def new_there(m, step, part):
        if step == steps:
            ref = new.at[m, 1, span(part, pos)]
        else:
            ref = new.at[m, 0, span(part, flipped(pos, step))]
        return remote(ref, ref, all_s.at[m, step, part], all_r.at[m, step, part], side)

    def last_step(m):
        return steps + 1 if m == TWO else steps

    def renew(m):
        send_sum(m, steps - 1).wait_recv()
        grad = total[m, starts[-1]] + landed[m, offset(steps - 1)].astype(jnp.float32)
        old = old_own[m]
        update = old - grad
        old_len = jnp.sqrt(jnp.sum(old * old, axis=1, keepdims=True))
        new_len = jnp.sqrt(jnp.sum(update * update, axis=1, keepdims=True) + EPS)
        new[m, 0, pos] = (update * (old_len / new_len)).astype(jnp.bfloat16)
        for step in range(last_step(m)):
            go(send_new(m, step, 0))

    pass_on(TWO, 1)
    keep_own(ONE)
    pass_on(ONE, 1)
    keep_own(THREE)
    pass_on(THREE, 1)
    keep_old(TWO)
    for step in range(2, steps):
        for m in order:
            pass_on(m, step)
    for m in order:
        renew(m)

    dim = width // ATT_HEADS
    scale = 1.0 / math.sqrt(dim)

    @pl.when(me != 0)
    def _():
        for copy in halo:
            copy.wait_recv()

    def attend(first_head, last_head):
        row = lax.broadcasted_iota(jnp.int32, (tokens, tokens), 0)
        col = lax.broadcasted_iota(jnp.int32, (tokens, tokens), 1)
        seg_row = seg_ref[...].astype(jnp.float32)
        seg_col = turned(seg_row, tokens)
        now_ok = (col <= row) & (row - col < WINDOW) & (seg_col == seg_row)
        old_ok = (
            (row - col + tokens < WINDOW)
            & (seg_col == old_seg[...].astype(jnp.float32))
            & (row + me * tokens >= row + tokens)
        )

        def one(i, carry):
            lanes = pl.ds(pl.multiple_of(i * dim, dim), dim)
            q = q_ref[:, lanes]

            def score(keys, allowed):
                return jnp.where(allowed, nt_dot(q, keys) * scale, jnp.float32(-1e30))

            old, now = score(old_k[:, lanes], old_ok), score(k_ref[:, lanes], now_ok)
            top = jnp.maximum(
                jnp.max(old, axis=1, keepdims=True), jnp.max(now, axis=1, keepdims=True)
            )
            old = jnp.where(old_ok, jnp.exp(old - top), jnp.float32(0.0))
            now = jnp.where(now_ok, jnp.exp(now - top), jnp.float32(0.0))
            norm = jnp.sum(old, axis=1, keepdims=True) + jnp.sum(now, axis=1, keepdims=True)
            out = dot((old / norm).astype(jnp.bfloat16), old_v[:, lanes]) + dot(
                (now / norm).astype(jnp.bfloat16), v_ref[:, lanes]
            )
            att_ref[:, lanes] = out.astype(jnp.bfloat16)
            return carry

        lax.fori_loop(first_head, last_head, one, 0)

    def mixed(place_from):
        slots = pl.ds(place_from * 2, 2)
        rows_q = qbuf[slots].reshape(2 * tokens, feats)
        b_one = asum[ONE, slots].reshape(2 * tokens, cols)
        b_three = nt_dot(rows_q, flat(new[THREE, 0]))
        return (jax.nn.silu(b_one) * b_three).astype(jnp.bfloat16)

    slots = len(order) * steps - 1
    for slot, (step, m) in enumerate((step, m) for step in range(steps) for m in order):
        for part in range(step + 1):
            new_there(m, step, part).wait_recv()
        for later in range(step + 1, last_step(m)):
            go(send_new(m, later, step + 1))
        if slot < slots:
            attend(ATT_HEADS * slot // slots, ATT_HEADS * (slot + 1) // slots)
        if (m, step) == (ONE, steps - 1):
            take_tokens(2)
            asum[ONE] = nt_dot(
                qbuf[...].reshape(4 * tokens, feats), flat(new[ONE, 0])
            ).reshape(4, tokens, cols)

    z_send[...] = mixed(1 - a)
    z_copy = remote(z_send, z_peer, end_s.at[0], end_r.at[0], pair)
    go(z_copy)
    z_own[...] = mixed(a)
    for part in range(steps + 1):
        new_there(TWO, steps, part).wait_recv()
    z_copy.wait_recv()

    def fast_rows(c):
        at = pl.ds(pl.multiple_of(c * tokens, tokens), tokens)
        value = dot(z_own[at, :], flat(new[TWO, 0])) + dot(z_peer[at, :], flat(new[TWO, 1]))
        return value.astype(jnp.bfloat16)

    o_send[...] = fast_rows(other)
    out_copy = remote(
        o_send, out_ref.at[:, own_lanes(core)], end_s.at[1], end_r.at[1], partner
    )
    go(out_copy)
    out_ref[:, own_lanes(core)] = fast_rows(core)
    theirs = out_ref.at[:, own_lanes(other)]
    remote(theirs, theirs, end_s.at[1], end_r.at[1], partner).wait_recv()

    for copy in started:
        copy.wait_send()
    for m in range(3):

        @pl.when(core == head)
        def _():
            for i in range(pairs(m)):
                to_mirror(m, i).wait_send()

        @pl.when(core != head)
        def _():
            first(m, 0).wait_send()

    @pl.when(me != count - 1)
    def _():
        for copy in halo:
            copy.wait_send()


def per_device(queries, keys, values, segment, rates, fast_one, fast_three, fast_two):
    count = lax.axis_size("tok")
    tokens, width = queries.shape
    rows, hidden = fast_one.shape
    lines = count // 8
    half = lines // 2
    steps = lines.bit_length()
    feats = width // FAST_HEADS
    cols = hidden // 2
    blocks = 2 * lines
    unit = cols // blocks
    bf16, f32 = jnp.bfloat16, jnp.float32
    dma = pltpu.SemaphoreType.DMA
    return pl.pallas_call(
        functools.partial(kernel, count),
        out_shape=[jax.ShapeDtypeStruct(queries.shape, bf16)] * 2,
        in_specs=[pl.BlockSpec(memory_space=pltpu.VMEM)] * 8,
        out_specs=[pl.BlockSpec(memory_space=pltpu.VMEM)] * 2,
        scratch_shapes=[
            pltpu.VMEM((3, count // 4, 2 * rows, cols), bf16),
            pltpu.VMEM((4, tokens, feats), bf16),
            pltpu.VMEM((4, tokens, feats), bf16),
            pltpu.VMEM((4, tokens, feats), bf16),
            pltpu.VMEM((4, 8, tokens), f32),
            pltpu.VMEM((FAST_HEADS, 8, tokens), f32),
            pltpu.VMEM((3, 4, tokens, cols), f32),
            pltpu.VMEM((3, cols, 4 * tokens), bf16),
            pltpu.VMEM((3, lines, unit, feats), f32),
            pltpu.VMEM((3, blocks, unit, feats), bf16),
            pltpu.VMEM((3, blocks, unit, feats), bf16),
            pltpu.VMEM((3, unit, feats), f32),
            pltpu.VMEM((lines, unit, feats), f32),
            pltpu.VMEM((3, 2, blocks, unit, feats), bf16),
            pltpu.VMEM((2 * tokens, cols), bf16),
            pltpu.VMEM((2 * tokens, cols), bf16),
            pltpu.VMEM((2 * tokens, cols), bf16),
            pltpu.VMEM((tokens, feats), bf16),
            pltpu.VMEM(keys.shape, bf16),
            pltpu.VMEM(values.shape, bf16),
            pltpu.VMEM((1, tokens), jnp.int32),
            dma((3, 4)),
            dma((3, 4, 2)),
            dma((3,)),
            dma((3, 2)),
            dma((3, 2)),
            dma((3, 2, half)),
            dma((3, 2, half)),
            dma((3, 2, half)),
            dma((3, 2, half)),
            dma((4, 3)),
            dma((4, 3)),
            dma((3, steps)),
            dma((3, steps)),
            dma((3, steps + 1, steps + 1)),
            dma((3, steps + 1, steps + 1)),
            dma((2,)),
            dma((2,)),
            dma((3,)),
            dma((3,)),
        ],
        compiler_params=pltpu.CompilerParams(
            collective_id=0, has_side_effects=True
        ),
    )(
        fast_one, fast_three, fast_two, queries, keys, values, segment.reshape(1, tokens), rates.T
    )


def solution(mesh):
    placed = P(("grp", "tok"), None)
    return jax.shard_map(
        per_device,
        mesh=mesh,
        in_specs=(placed, placed, placed, P(("grp", "tok")), placed, placed, placed, placed),
        out_specs=(placed, placed),
        check_vma=False,
    )
```

```python
import functools
import math

import jax
import jax.numpy as jnp
from jax import lax
from jax.experimental import pallas as pl
from jax.experimental.pallas import tpu as pltpu
from jax.sharding import PartitionSpec as P

ATT_HEADS = 16
FAST_HEADS = 2
WINDOW = 128
EPS = 1e-06

ONE, THREE, TWO = 0, 1, 2
WIDE = (TWO,)
SPLIT = 2


def device(line, x, y, core):
    return ((line * 2 + y) * 2 + x) * 2 + core


def in_role(line, a, b, role):
    return device(line, a + role * (b - a), b + role * (a - b), role)


def bit_of(index, bit):
    return lax.rem(lax.div(index, jnp.int32(1 << bit)), jnp.int32(2))


def flipped(index, bit):
    return index + (1 - 2 * bit_of(index, bit)) * (1 << bit)


def remote(src, dst, send_sem, recv_sem, partner):
    return pltpu.make_async_remote_copy(
        src_ref=src,
        dst_ref=dst,
        send_sem=send_sem,
        recv_sem=recv_sem,
        device_id={"tok": partner},
        device_id_type=pl.DeviceIdType.MESH,
    )


def turned(row, size):
    return jnp.transpose(jnp.broadcast_to(row, (size, size)))


def nt_dot(left, right):
    return lax.dot_general(
        left, right, (((1,), (1,)), ((), ())), preferred_element_type=jnp.float32
    )


def dot(left, right):
    return jnp.dot(left, right, preferred_element_type=jnp.float32)


def flat(blocks):
    n, unit, width = blocks.shape
    if unit % 16 == 0:
        return blocks.reshape(n * unit, width)
    return blocks.astype(jnp.float32).reshape(n * unit, width).astype(jnp.bfloat16)


def kernel(count, *refs):
    att_ref, out_ref = refs[8:10]
    loaded, load_sem = refs[10:18], refs[18]
    w_refs = loaded[:3]
    q_ref, k_ref, v_ref, seg_ref, rate_ref = loaded[3:8]
    (
        wbuf, kbuf, vbuf, qbuf, rbuf, rsend, asum, hid, total, staged, landed, old_own, old_all, new,
        z_own, z_peer, z_send, o_send, old_k, old_v, old_seg,
        first_s, first_r, first_l, mirror_s, mirror_r, mate_s, mate_r, side_s, side_r,
        tok_s, tok_r, sum_s, sum_r, all_s, all_r, end_s, end_r, halo_s, halo_r,
    ) = refs[19:]

    lines = count // 8
    half = lines // 2
    line_bits = lines.bit_length() - 1
    steps = line_bits + 1
    rows, hidden = w_refs[0].shape
    cols = hidden // 2
    tokens, width = q_ref.shape
    feats = width // FAST_HEADS
    blocks = 2 * lines
    unit = cols // blocks
    wide = feats // SPLIT

    def parts(m):
        return range(m * SPLIT, (m + 1) * SPLIT)

    def lanes_of(v):
        return slice(v % SPLIT * wide, (v % SPLIT + 1) * wide)

    me = lax.axis_index("tok")
    core, chip = lax.rem(me, 2), lax.div(me, 2)
    x, y, line = lax.rem(chip, 2), lax.rem(lax.div(chip, 2), 2), lax.div(chip, 4)
    a, b = x + core * (y - x), y + core * (x - y)
    a_other, b_other = b, a
    other = 1 - core
    partner = device(line, x, y, other)
    pair = in_role(line, 1 - a, b, core)
    side = in_role(line, a, 1 - b, core)
    pair_takes = in_role(line, 1 - a_other, b_other, other)
    mirror_line = lax.rem(line + half, lines)
    mirror = in_role(mirror_line, a, b, core)
    upper = lax.div(line, half)
    place = line - upper * half
    base = upper * half

    def mate(i):
        return in_role(base + lax.rem(place + i, half), a, b, core)

    def around(i):
        return lax.rem(me + count + i, count)

    after = around(1)
    loads = [pltpu.make_async_copy(refs[i], loaded[i], load_sem.at[i]) for i in range(8)]
    loading = (0, 1, 2, 4, 7, 5, 6, 3)
    for i in loading:
        loads[i].start()

    barrier = pltpu.get_barrier_semaphore()
    plane = line * 8
    known = [plane + lax.rem(me - plane + i, 8) for i in range(1, 8)]
    known += [mirror] + [mate(i) for i in range(1, half)]
    known += [around(i) for i in (1, -1, 4, -4, 5, -5)]
    for one in known:
        pl.semaphore_signal(
            barrier, inc=1, device_id={"tok": one}, device_id_type=pl.DeviceIdType.MESH
        )
    for i in loading:
        loads[i].wait()
    for group in range(FAST_HEADS):
        rsend[group] = jnp.broadcast_to(rate_ref[group : group + 1, :], (8, tokens))
    pl.semaphore_wait(barrier, len(known))

    started = []

    def go(copy):
        copy.start()
        started.append(copy)

    head = upper
    head_a, head_b = x + head * (y - x), y + head * (x - y)
    stored = place * 4 + y * 2 + x

    def first(m, far):
        cross, apart = far % 2, far // 2
        start = (head_a + cross - 2 * cross * head_a) * cols
        src = w_refs[m].at[:, pl.ds(pl.multiple_of(start, cols), cols)]
        dst = wbuf.at[m, stored, pl.ds(pl.multiple_of(core * rows, rows), rows), :]
        to_a = 1 - head_a if cross else head_a
        to = in_role(line, to_a, 1 - head_b if apart else head_b, head)
        return remote(src, dst, first_s.at[m, far], first_r.at[m, far, core], to)

    def first_here(m):
        src = w_refs[m].at[:, pl.ds(pl.multiple_of(head_a * cols, cols), cols)]
        dst = wbuf.at[m, stored, pl.ds(pl.multiple_of(core * rows, rows), rows), :]
        return pltpu.make_async_copy(src, dst, first_l.at[m])

    def reach(m):
        return 4 if m in WIDE else 2

    for m in range(3):
        for far in range(1, reach(m)):
            go(first(m, far))

        @pl.when(core == head)
        def _():
            first_here(m).start()

        @pl.when(core != head)
        def _():
            first(m, 0).start()

    def own_lanes(group):
        return pl.ds(pl.multiple_of(group * feats, feats), feats)

    def send_tokens(kind):
        ref, buf = ((k_ref, kbuf), (v_ref, vbuf), (q_ref, qbuf), (rsend, rbuf))[kind]
        if kind == 3:
            mine, theirs = ref.at[core], ref.at[other]
        else:
            mine, theirs = ref.at[:, own_lanes(core)], ref.at[:, own_lanes(other)]
        here, there = buf.at[a * 2 + core], buf.at[a_other * 2 + core]
        go(remote(mine, here, tok_s.at[kind, 0], tok_r.at[kind, 1 + core], pair))
        go(remote(theirs, there, tok_s.at[kind, 1], tok_r.at[kind, 0], partner))
        go(remote(theirs, there, tok_s.at[kind, 2], tok_r.at[kind, 1 + core], pair_takes))
        if kind == 3:
            rbuf[a * 2 + core] = rsend[core]
        else:
            buf[a * 2 + core] = ref[:, own_lanes(core)]

    def take_tokens(kind):
        buf = (kbuf, vbuf, qbuf, rbuf)[kind]
        for i, slot in ((0, a * 2 + other), (1, (1 - a) * 2), (2, (1 - a) * 2 + 1)):
            ref = buf.at[slot]
            remote(ref, ref, tok_s.at[kind, i], tok_r.at[kind, i], partner).wait_recv()

    send_tokens(0)
    send_tokens(3)
    send_tokens(1)

    def pairs(m):
        return 1 if m in WIDE else 2

    def piece(m, k, i, b_from):
        if m in WIDE:
            return wbuf.at[m, pl.ds(k * 4, 4)]
        return wbuf.at[m, k * 4 + b_from * 2 + i + core * (i - b_from)]

    def first_wait(m):
        first_here(m).wait()
        for far in range(reach(m)):
            from_a = 1 - a if far % 2 else a
            from_b = 1 - b if far // 2 else b
            block = wbuf.at[m, place * 4 + from_b * 2 + from_a + core * (from_a - from_b)]
            for c in (other,) if far == 0 else (0, 1):
                ref = block.at[pl.ds(pl.multiple_of(c * rows, rows), rows), :]
                copy = remote(ref, ref, first_s.at[m, far], first_r.at[m, far, c], partner)
                copy.wait_recv()

    def to_mirror(m, i):
        ref = piece(m, place, i, b)
        return remote(ref, ref, mirror_s.at[m, i], mirror_r.at[m, i], mirror)

    def to_mate(m, i, step):
        ref = piece(m, place, i, b)
        return remote(ref, ref, mate_s.at[m, i, step], mate_r.at[m, i, step], mate(step))

    def from_mate(m, i, step):
        ref = piece(m, lax.rem(place + half - step, half), i, b)
        return remote(ref, ref, mate_s.at[m, i, step], mate_r.at[m, i, step], mate(step))

    def to_side(m, i, step):
        ref = piece(m, lax.rem(place + half - step, half), i, b)
        return remote(ref, ref, side_s.at[m, i, step], side_r.at[m, i, step], side)

    def from_side(m, i, step):
        ref = piece(m, lax.rem(place + half - step, half), i, 1 - b)
        return remote(ref, ref, side_s.at[m, i, step], side_r.at[m, i, step], side)

    for m in range(3):

        @pl.when(core == head)
        def _():
            first_wait(m)
            for i in range(pairs(m)):
                to_mirror(m, i).start()

        @pl.when(core != head)
        def _():
            for i in range(pairs(m)):
                to_mirror(m, i).wait_recv()

        for i in range(pairs(m)):
            for step in range(1, half):
                go(to_mate(m, i, step))
            if m not in WIDE:
                go(to_side(m, i, 0))
    for m in range(3):
        if m in WIDE:
            continue
        for step in range(1, half):
            for i in range(2):
                from_mate(m, i, step).wait_recv()
                go(to_side(m, i, step))

    def weight_there(m):
        if m in WIDE:
            for step in range(1, half):
                from_mate(m, 0, step).wait_recv()
            return
        for step in range(half):
            for i in range(2):
                from_side(m, i, step).wait_recv()

    def weight(m):
        return wbuf[m].reshape(feats, cols)

    all_keys = lambda: kbuf[...].reshape(4 * tokens, feats)
    all_values = lambda: vbuf[...].reshape(4 * tokens, feats)

    def part_of(which):
        return pl.ds(pl.multiple_of(which * (cols // 2), cols // 2), cols // 2)

    def spread(s):
        column = turned(rbuf[s][0:1, :], tokens)
        return jnp.concatenate([column] * (cols // 2 // tokens), axis=1)

    def keep(m, s, which, value):
        lanes = pl.ds(pl.multiple_of(s * tokens, tokens), tokens)
        hid[m, part_of(which), lanes] = jnp.transpose(value).astype(jnp.bfloat16)

    def weigh(which):
        def one(s, carry):
            a_one, a_three = asum[ONE, s, :, part_of(which)], asum[THREE, s, :, part_of(which)]
            keep(TWO, s, which, -spread(s) * a_one * jax.nn.sigmoid(a_one) * a_three)
            return carry

        lax.fori_loop(0, 4, one, 0)

    line_bit = [bit_of(line, i) for i in range(line_bits)]
    starts = [jnp.int32(0)]
    for i in range(line_bits):
        starts.append(starts[-1] + line_bit[i] * (lines >> (i + 1)))
    pos = b * lines + starts[-1]

    def gradient(v, which):
        m = v // SPLIT
        ref = vbuf if m == TWO else kbuf
        side_rows = ref[:, :, lanes_of(v)].reshape(4 * tokens, wide)
        return dot(hid[m, part_of(which), :], side_rows).reshape(lines, unit, wide)

    def offset(step):
        return blocks - 2 * (lines >> step)

    def send_sum(m, step):
        at = pl.ds(offset(step), lines >> step)
        to = side if step == 0 else in_role(flipped(line, step - 1), a, b, core)
        return remote(
            staged.at[m, at], landed.at[m, at], sum_s.at[m, step], sum_r.at[m, step], to
        )

    def send_away(m):
        for v in parts(m):
            staged[v, pl.ds(0, lines)] = gradient(v, 1 - b).astype(jnp.bfloat16)
            go(send_sum(v, 0))

    def keep_own(m):
        for v in parts(m):
            total[v] = gradient(v, b)

    def keep_old(m):
        lanes = pl.ds(pl.multiple_of(b * (cols // 2), cols // 2), cols // 2)
        mine = wbuf[m, :, :, lanes].reshape(feats, cols // 2).astype(jnp.float32)
        old_all[...] = jnp.transpose(mine).reshape(lines, unit, feats)
        old_own[m] = old_all[starts[-1]]

    def deltas(which):
        def one(s, carry):
            a_one, a_three = asum[ONE, s, :, part_of(which)], asum[THREE, s, :, part_of(which)]
            back = -spread(s) * asum[TWO, s, :, part_of(which)]
            sig = jax.nn.sigmoid(a_one)
            keep(ONE, s, which, back * a_three * sig * (1.0 + a_one * (1.0 - sig)))
            keep(THREE, s, which, back * a_one * sig)
            return carry

        lax.fori_loop(0, 4, one, 0)

    def project(m):
        weight_there(m)
        rows_in = all_values() if m == TWO else all_keys()
        asum[m] = dot(rows_in, weight(m)).reshape(4, tokens, cols)

    take_tokens(0)
    take_tokens(3)
    project(ONE)
    project(THREE)
    weigh(1 - b)
    take_tokens(1)
    send_away(TWO)
    weigh(b)
    keep_own(TWO)
    keep_old(ONE)
    keep_old(THREE)
    project(TWO)
    deltas(1 - b)
    send_away(ONE)
    send_away(THREE)
    send_tokens(2)

    seg_copy = remote(seg_ref, old_seg, halo_s.at[4], halo_r.at[4], after)
    kinds = ((k_ref, kbuf, old_k), (v_ref, vbuf, old_v))

    def halo(i, group):
        ref, buf, old = kinds[i]
        if group is None:
            return remote(ref, old, halo_s.at[i], halo_r.at[i], partner)
        at = old.at[:, pl.ds(group * feats, feats)]
        if group == 0:
            slot, to = 3, device(lax.rem(line + y, lines), 0, 1 - y, 0)
        else:
            slot = (y + x - 2 * x * y) * 2 + 1
            to = device(lax.rem(line + x * (1 - y), lines), 1 - x, y, 0)
        return remote(buf.at[slot], at, halo_s.at[i * 2 + group], halo_r.at[i * 2 + group], to)

    def halo_from(i, group):
        ref, buf, old = kinds[i]
        if group is None:
            return halo(i, None)
        at = old.at[:, pl.ds(group * feats, feats)]
        return remote(at, at, halo_s.at[i * 2 + group], halo_r.at[i * 2 + group], partner)

    last_line = line == lines - 1
    sends_zero = (core == 0) & (x == 0) & jnp.logical_not((y == 1) & last_line)
    sends_one = (core == 1) & jnp.logical_not((x == 1) & (y == 0) & last_line)

    def each_halo(act_inner, act_zero, act_one, act_seg, inner, zero, one, seg):
        @pl.when(inner)
        def _():
            for i in range(2):
                act_inner(i)

        @pl.when(zero)
        def _():
            for i in range(2):
                act_zero(i)

        @pl.when(one)
        def _():
            for i in range(2):
                act_one(i)

        @pl.when(seg)
        def _():
            act_seg()

    each_halo(
        lambda i: halo(i, None).start(),
        lambda i: halo(i, 0).start(),
        lambda i: halo(i, 1).start(),
        seg_copy.start,
        core == 0,
        sends_zero,
        sends_one,
        me != count - 1,
    )

    @pl.when(me == 0)
    def _():
        old_k[...] = jnp.zeros_like(old_k)
        old_v[...] = jnp.zeros_like(old_v)
        old_seg[...] = jnp.zeros_like(old_seg)

    @pl.when((core == 0) & (x == 1))
    def _():
        for _, buf, old in kinds:
            old[:, 0:feats] = buf[1]

    order = (TWO, ONE, THREE)

    def pass_on(m, step):
        size = lines >> step
        bit = line_bit[step - 1]
        kept, away = starts[step], starts[step - 1] + (1 - bit) * size
        shift = offset(step - 1) - starts[step - 1]
        send_sum(m, step - 1).wait_recv()

        def stage(i, carry):
            value = total[m, away + i] + landed[m, shift + away + i].astype(jnp.float32)
            staged[m, offset(step) + i] = value.astype(jnp.bfloat16)
            return carry

        def hold(i, carry):
            value = total[m, kept + i] + landed[m, shift + kept + i].astype(jnp.float32)
            total[m, kept + i] = value
            return carry

        lax.fori_loop(0, size, stage, 0)
        go(send_sum(m, step))
        lax.fori_loop(0, size, hold, 0)

    def pass_all(m, step):
        for v in parts(m):
            pass_on(v, step)

    def span(part, position):
        if part == 0:
            return pl.ds(position, 1)
        size = 1 << (part - 1)
        return pl.ds(flipped(lax.div(position, jnp.int32(size)), 0) * size, size)

    def send_new(m, step, part):
        src = new.at[m, 0, span(part, pos)]
        if step == steps:
            dst, to = new.at[m, 1, span(part, pos)], pair
        elif step == steps - 1:
            dst, to = src, side
        else:
            dst, to = src, in_role(flipped(line, line_bits - 1 - step), a, b, core)
        return remote(src, dst, all_s.at[m, step, part], all_r.at[m, step, part], to)

    def new_there(m, step, part):
        if step == steps:
            ref = new.at[m, 1, span(part, pos)]
        else:
            ref = new.at[m, 0, span(part, flipped(pos, step))]
        return remote(ref, ref, all_s.at[m, step, part], all_r.at[m, step, part], side)

    def last_step(v):
        return steps + 1 if v // SPLIT == TWO else steps

    def renew(m):
        updates, square = [], 0.0
        for v in parts(m):
            send_sum(v, steps - 1).wait_recv()
            grad = total[v, starts[-1]] + landed[v, offset(steps - 1)].astype(jnp.float32)
            updates.append(old_own[m, :, lanes_of(v)] - grad)
            square += jnp.sum(updates[-1] * updates[-1], axis=1, keepdims=True)
        old = old_own[m]
        old_len = jnp.sqrt(jnp.sum(old * old, axis=1, keepdims=True))
        ratio = old_len / jnp.sqrt(square + EPS)
        for v, update in zip(parts(m), updates):
            new[v, 0, pos] = (update * ratio).astype(jnp.bfloat16)
            for step in range(last_step(v)):
                go(send_new(v, step, 0))

    pass_all(TWO, 1)
    deltas(b)
    keep_own(ONE)
    pass_all(ONE, 1)
    keep_own(THREE)
    pass_all(THREE, 1)
    keep_old(TWO)
    for step in range(2, steps):
        for m in order:
            pass_all(m, step)
    for m in order:
        renew(m)

    dim = width // ATT_HEADS
    scale = 1.0 / math.sqrt(dim)

    each_halo(
        lambda i: halo_from(i, None).wait_recv(),
        lambda i: halo_from(i, 0).wait_recv(),
        lambda i: halo_from(i, 1).wait_recv(),
        seg_copy.wait_recv,
        core == 1,
        (core == 0) & (x == 0) & (me != 0),
        (core == 0) & (me != 0),
        me != 0,
    )

    def attend(first_head, last_head):
        row = lax.broadcasted_iota(jnp.int32, (tokens, tokens), 0)
        col = lax.broadcasted_iota(jnp.int32, (tokens, tokens), 1)
        seg_row = seg_ref[...].astype(jnp.float32)
        seg_col = turned(seg_row, tokens)
        now_ok = (col <= row) & (row - col < WINDOW) & (seg_col == seg_row)
        old_ok = (
            (row - col + tokens < WINDOW)
            & (seg_col == old_seg[...].astype(jnp.float32))
            & (row + me * tokens >= row + tokens)
        )

        def one(i, carry):
            lanes = pl.ds(pl.multiple_of(i * dim, dim), dim)
            q = q_ref[:, lanes]

            def score(keys, allowed):
                return jnp.where(allowed, nt_dot(q, keys) * scale, jnp.float32(-1e30))

            old, now = score(old_k[:, lanes], old_ok), score(k_ref[:, lanes], now_ok)
            top = jnp.maximum(
                jnp.max(old, axis=1, keepdims=True), jnp.max(now, axis=1, keepdims=True)
            )
            old = jnp.where(old_ok, jnp.exp(old - top), jnp.float32(0.0))
            now = jnp.where(now_ok, jnp.exp(now - top), jnp.float32(0.0))
            norm = jnp.sum(old, axis=1, keepdims=True) + jnp.sum(now, axis=1, keepdims=True)
            out = dot((old / norm).astype(jnp.bfloat16), old_v[:, lanes]) + dot(
                (now / norm).astype(jnp.bfloat16), v_ref[:, lanes]
            )
            att_ref[:, lanes] = out.astype(jnp.bfloat16)
            return carry

        lax.fori_loop(first_head, last_head, one, 0)

    def query_dot(m, rows_q):
        return sum(nt_dot(rows_q[:, lanes_of(v)], flat(new[v, 0])) for v in parts(m))

    def mixed(place_from):
        slots = pl.ds(place_from * 2, 2)
        b_one = asum[ONE, slots].reshape(2 * tokens, cols)
        b_three = query_dot(THREE, qbuf[slots].reshape(2 * tokens, feats))
        return (jax.nn.silu(b_one) * b_three).astype(jnp.bfloat16)

    turns = [(step, m, v) for step in range(steps) for m in order for v in parts(m)]
    slots = len(turns) - 2
    for slot, (step, m, v) in enumerate(turns):
        for part in range(step + 1):
            new_there(v, step, part).wait_recv()
        for later in range(step + 1, last_step(v)):
            go(send_new(v, later, step + 1))
        if slot < slots:
            attend(ATT_HEADS * slot // slots, ATT_HEADS * (slot + 1) // slots)
        if (step, v) == (steps - 1, parts(ONE)[-1]):
            take_tokens(2)
            rows_q = qbuf[...].reshape(4 * tokens, feats)
            asum[ONE] = query_dot(ONE, rows_q).reshape(4, tokens, cols)

    z_send[...] = mixed(1 - a)
    z_copy = remote(z_send, z_peer, end_s.at[0], end_r.at[0], pair)
    go(z_copy)
    z_own[...] = mixed(a)
    for v in parts(TWO):
        for part in range(steps + 1):
            new_there(v, steps, part).wait_recv()
    z_copy.wait_recv()

    def fast_rows(c, v):
        at = pl.ds(pl.multiple_of(c * tokens, tokens), tokens)
        value = dot(z_own[at, :], flat(new[v, 0])) + dot(z_peer[at, :], flat(new[v, 1]))
        return value.astype(jnp.bfloat16)

    for v in parts(TWO):
        o_send[:, lanes_of(v)] = fast_rows(other, v)
    out_copy = remote(
        o_send, out_ref.at[:, own_lanes(core)], end_s.at[1], end_r.at[1], partner
    )
    go(out_copy)
    for v in parts(TWO):
        lanes = pl.ds(pl.multiple_of(core * feats + v % SPLIT * wide, wide), wide)
        out_ref[:, lanes] = fast_rows(core, v)
    theirs = out_ref.at[:, own_lanes(other)]
    remote(theirs, theirs, end_s.at[1], end_r.at[1], partner).wait_recv()

    for copy in started:
        copy.wait_send()
    for m in range(3):

        @pl.when(core == head)
        def _():
            for i in range(pairs(m)):
                to_mirror(m, i).wait_send()

        @pl.when(core != head)
        def _():
            first(m, 0).wait_send()

    each_halo(
        lambda i: halo(i, None).wait_send(),
        lambda i: halo(i, 0).wait_send(),
        lambda i: halo(i, 1).wait_send(),
        seg_copy.wait_send,
        core == 0,
        sends_zero,
        sends_one,
        me != count - 1,
    )


def per_device(queries, keys, values, segment, rates, fast_one, fast_three, fast_two):
    count = lax.axis_size("tok")
    tokens, width = queries.shape
    rows, hidden = fast_one.shape
    lines = count // 8
    half = lines // 2
    steps = lines.bit_length()
    feats = width // FAST_HEADS
    cols = hidden // 2
    blocks = 2 * lines
    unit = cols // blocks
    wide = feats // SPLIT
    bf16, f32 = jnp.bfloat16, jnp.float32
    dma = pltpu.SemaphoreType.DMA
    operands = (
        fast_one, fast_three, fast_two, queries, keys, values, segment.reshape(1, tokens), rates.T
    )
    return pl.pallas_call(
        functools.partial(kernel, count),
        out_shape=[jax.ShapeDtypeStruct(queries.shape, bf16)] * 2,
        in_specs=[pl.BlockSpec(memory_space=pltpu.HBM)] * 8,
        out_specs=[pl.BlockSpec(memory_space=pltpu.VMEM)] * 2,
        scratch_shapes=[pltpu.VMEM(one.shape, one.dtype) for one in operands]
        + [
            dma((8,)),
            pltpu.VMEM((3, count // 4, 2 * rows, cols), bf16),
            pltpu.VMEM((4, tokens, feats), bf16),
            pltpu.VMEM((4, tokens, feats), bf16),
            pltpu.VMEM((4, tokens, feats), bf16),
            pltpu.VMEM((4, 8, tokens), f32),
            pltpu.VMEM((FAST_HEADS, 8, tokens), f32),
            pltpu.VMEM((3, 4, tokens, cols), f32),
            pltpu.VMEM((3, cols, 4 * tokens), bf16),
            pltpu.VMEM((3 * SPLIT, lines, unit, wide), f32),
            pltpu.VMEM((3 * SPLIT, blocks, unit, wide), bf16),
            pltpu.VMEM((3 * SPLIT, blocks, unit, wide), bf16),
            pltpu.VMEM((3, unit, feats), f32),
            pltpu.VMEM((lines, unit, feats), f32),
            pltpu.VMEM((3 * SPLIT, 2, blocks, unit, wide), bf16),
            pltpu.VMEM((2 * tokens, cols), bf16),
            pltpu.VMEM((2 * tokens, cols), bf16),
            pltpu.VMEM((2 * tokens, cols), bf16),
            pltpu.VMEM((tokens, feats), bf16),
            pltpu.VMEM(keys.shape, bf16),
            pltpu.VMEM(values.shape, bf16),
            pltpu.VMEM((1, tokens), jnp.int32),
            dma((3, 4)),
            dma((3, 4, 2)),
            dma((3,)),
            dma((3, 2)),
            dma((3, 2)),
            dma((3, 2, half)),
            dma((3, 2, half)),
            dma((3, 2, half)),
            dma((3, 2, half)),
            dma((4, 3)),
            dma((4, 3)),
            dma((3 * SPLIT, steps)),
            dma((3 * SPLIT, steps)),
            dma((3 * SPLIT, steps + 1, steps + 1)),
            dma((3 * SPLIT, steps + 1, steps + 1)),
            dma((2,)),
            dma((2,)),
            dma((5,)),
            dma((5,)),
        ],
        compiler_params=pltpu.CompilerParams(
            collective_id=0, has_side_effects=True, vmem_limit_bytes=40 << 20
        ),
    )(*[pltpu.with_memory_space_constraint(one, pltpu.HBM) for one in operands])


def solution(mesh):
    placed = P(("grp", "tok"), None)
    return jax.shard_map(
        per_device,
        mesh=mesh,
        in_specs=(placed, placed, placed, P(("grp", "tok")), placed, placed, placed, placed),
        out_specs=(placed, placed),
        check_vma=False,
    )
```

```python
import functools
import math

import jax
import jax.numpy as jnp
from jax import lax
from jax.experimental import pallas as pl
from jax.experimental.pallas import tpu as pltpu
from jax.sharding import PartitionSpec as P

ATT_HEADS = 16
FAST_HEADS = 2
WINDOW = 128
EPS = 1e-06

ONE, THREE, TWO = 0, 1, 2
WIDE = (TWO,)
SPLIT = 2


def device(line, x, y, core):
    return ((line * 2 + y) * 2 + x) * 2 + core


def in_role(line, a, b, role):
    return device(line, a + role * (b - a), b + role * (a - b), role)


def bit_of(index, bit):
    return lax.rem(lax.div(index, jnp.int32(1 << bit)), jnp.int32(2))


def flipped(index, bit):
    return index + (1 - 2 * bit_of(index, bit)) * (1 << bit)


def remote(src, dst, send_sem, recv_sem, partner):
    return pltpu.make_async_remote_copy(
        src_ref=src,
        dst_ref=dst,
        send_sem=send_sem,
        recv_sem=recv_sem,
        device_id={"tok": partner},
        device_id_type=pl.DeviceIdType.MESH,
    )


def turned(row, size):
    return jnp.transpose(jnp.broadcast_to(row, (size, size)))


def nt_dot(left, right):
    return lax.dot_general(
        left, right, (((1,), (1,)), ((), ())), preferred_element_type=jnp.float32
    )


def dot(left, right):
    return jnp.dot(left, right, preferred_element_type=jnp.float32)


def flat(blocks):
    n, unit, width = blocks.shape
    if unit % 16 == 0:
        return blocks.reshape(n * unit, width)
    return blocks.astype(jnp.float32).reshape(n * unit, width).astype(jnp.bfloat16)


def kernel(count, *refs):
    att_ref, out_ref = refs[8:10]
    loaded, load_sem = refs[10:18], refs[18]
    w_refs = loaded[:3]
    q_ref, k_ref, v_ref, seg_ref, rate_ref = loaded[3:8]
    (
        wbuf, kbuf, vbuf, qbuf, rbuf, rsend, asum, hid, total, staged, landed, old_own, old_all, new,
        z_own, z_peer, z_send, o_send, old_k, old_v, old_seg, relay,
        first_s, first_r, first_l, mirror_s, mirror_r, mate_s, mate_r, side_s, side_r,
        tok_s, tok_r, sum_s, sum_r, all_s, all_r, end_s, end_r, halo_s, halo_r, up_s, up_r,
    ) = refs[19:]

    lines = count // 8
    half = lines // 2
    line_bits = lines.bit_length() - 1
    steps = line_bits + 1
    rows, hidden = w_refs[0].shape
    cols = hidden // 2
    tokens, width = q_ref.shape
    feats = width // FAST_HEADS
    blocks = 2 * lines
    unit = cols // blocks
    wide = feats // SPLIT

    def parts(m):
        return range(m * SPLIT, (m + 1) * SPLIT)

    def lanes_of(v):
        return slice(v % SPLIT * wide, (v % SPLIT + 1) * wide)

    me = lax.axis_index("tok")
    core, chip = lax.rem(me, 2), lax.div(me, 2)
    x, y, line = lax.rem(chip, 2), lax.rem(lax.div(chip, 2), 2), lax.div(chip, 4)
    a, b = x + core * (y - x), y + core * (x - y)
    a_other, b_other = b, a
    other = 1 - core
    partner = device(line, x, y, other)
    pair = in_role(line, 1 - a, b, core)
    side = in_role(line, a, 1 - b, core)
    pair_takes = in_role(line, 1 - a_other, b_other, other)
    mirror_line = lax.rem(line + half, lines)
    mirror = in_role(mirror_line, a, b, core)
    upper = lax.div(line, half)
    place = line - upper * half
    base = upper * half

    def mate(i):
        return in_role(base + lax.rem(place + i, half), a, b, core)

    def around(i):
        return lax.rem(me + count + i, count)

    after = around(1)
    loads = [pltpu.make_async_copy(refs[i], loaded[i], load_sem.at[i]) for i in range(8)]
    loading = (0, 1, 2, 4, 7, 5, 6, 3)
    for i in loading:
        loads[i].start()

    barrier = pltpu.get_barrier_semaphore()
    plane = line * 8
    known = [plane + lax.rem(me - plane + i, 8) for i in range(1, 8)]
    known += [mirror] + [mate(i) for i in range(1, half)]
    known += [around(i) for i in (1, -1, 8, -8)]
    for one in known:
        pl.semaphore_signal(
            barrier, inc=1, device_id={"tok": one}, device_id_type=pl.DeviceIdType.MESH
        )
    for i in loading:
        loads[i].wait()
    for group in range(FAST_HEADS):
        rsend[group] = jnp.broadcast_to(rate_ref[group : group + 1, :], (8, tokens))
    pl.semaphore_wait(barrier, len(known))

    started = []

    def go(copy):
        copy.start()
        started.append(copy)

    head = upper
    head_a, head_b = x + head * (y - x), y + head * (x - y)
    stored = place * 4 + y * 2 + x

    def first(m, far):
        cross, apart = far % 2, far // 2
        start = (head_a + cross - 2 * cross * head_a) * cols
        src = w_refs[m].at[:, pl.ds(pl.multiple_of(start, cols), cols)]
        dst = wbuf.at[m, stored, pl.ds(pl.multiple_of(core * rows, rows), rows), :]
        to_a = 1 - head_a if cross else head_a
        to = in_role(line, to_a, 1 - head_b if apart else head_b, head)
        return remote(src, dst, first_s.at[m, far], first_r.at[m, far, core], to)

    def first_here(m):
        src = w_refs[m].at[:, pl.ds(pl.multiple_of(head_a * cols, cols), cols)]
        dst = wbuf.at[m, stored, pl.ds(pl.multiple_of(core * rows, rows), rows), :]
        return pltpu.make_async_copy(src, dst, first_l.at[m])

    def reach(m):
        return 4 if m in WIDE else 2

    for m in range(3):
        for far in range(1, reach(m)):
            go(first(m, far))

        @pl.when(core == head)
        def _():
            first_here(m).start()

        @pl.when(core != head)
        def _():
            first(m, 0).start()

    def own_lanes(group):
        return pl.ds(pl.multiple_of(group * feats, feats), feats)

    def send_tokens(kind):
        ref, buf = ((k_ref, kbuf), (v_ref, vbuf), (q_ref, qbuf), (rsend, rbuf))[kind]
        if kind == 3:
            mine, theirs = ref.at[core], ref.at[other]
        else:
            mine, theirs = ref.at[:, own_lanes(core)], ref.at[:, own_lanes(other)]
        here, there = buf.at[a * 2 + core], buf.at[a_other * 2 + core]
        go(remote(mine, here, tok_s.at[kind, 0], tok_r.at[kind, 1 + core], pair))
        go(remote(theirs, there, tok_s.at[kind, 1], tok_r.at[kind, 0], partner))
        go(remote(theirs, there, tok_s.at[kind, 2], tok_r.at[kind, 1 + core], pair_takes))
        if kind == 3:
            rbuf[a * 2 + core] = rsend[core]
        else:
            buf[a * 2 + core] = ref[:, own_lanes(core)]

    def take_tokens(kind):
        buf = (kbuf, vbuf, qbuf, rbuf)[kind]
        for i, slot in ((0, a * 2 + other), (1, (1 - a) * 2), (2, (1 - a) * 2 + 1)):
            ref = buf.at[slot]
            remote(ref, ref, tok_s.at[kind, i], tok_r.at[kind, i], partner).wait_recv()

    send_tokens(0)
    send_tokens(3)
    send_tokens(1)

    def pairs(m):
        return 1 if m in WIDE else 2

    def piece(m, k, i, b_from):
        if m in WIDE:
            return wbuf.at[m, pl.ds(k * 4, 4)]
        return wbuf.at[m, k * 4 + b_from * 2 + i + core * (i - b_from)]

    def first_wait(m):
        first_here(m).wait()
        for far in range(reach(m)):
            from_a = 1 - a if far % 2 else a
            from_b = 1 - b if far // 2 else b
            block = wbuf.at[m, place * 4 + from_b * 2 + from_a + core * (from_a - from_b)]
            for c in (other,) if far == 0 else (0, 1):
                ref = block.at[pl.ds(pl.multiple_of(c * rows, rows), rows), :]
                copy = remote(ref, ref, first_s.at[m, far], first_r.at[m, far, c], partner)
                copy.wait_recv()

    def to_mirror(m, i):
        ref = piece(m, place, i, b)
        return remote(ref, ref, mirror_s.at[m, i], mirror_r.at[m, i], mirror)

    def to_mate(m, i, step):
        ref = piece(m, place, i, b)
        return remote(ref, ref, mate_s.at[m, i, step], mate_r.at[m, i, step], mate(step))

    def from_mate(m, i, step):
        ref = piece(m, lax.rem(place + half - step, half), i, b)
        return remote(ref, ref, mate_s.at[m, i, step], mate_r.at[m, i, step], mate(step))

    def to_side(m, i, step):
        ref = piece(m, lax.rem(place + half - step, half), i, b)
        return remote(ref, ref, side_s.at[m, i, step], side_r.at[m, i, step], side)

    def from_side(m, i, step):
        ref = piece(m, lax.rem(place + half - step, half), i, 1 - b)
        return remote(ref, ref, side_s.at[m, i, step], side_r.at[m, i, step], side)

    for m in range(3):

        @pl.when(core == head)
        def _():
            first_wait(m)
            for i in range(pairs(m)):
                to_mirror(m, i).start()

        @pl.when(core != head)
        def _():
            for i in range(pairs(m)):
                to_mirror(m, i).wait_recv()

        for i in range(pairs(m)):
            for step in range(1, half):
                go(to_mate(m, i, step))
            if m not in WIDE:
                go(to_side(m, i, 0))
    for m in range(3):
        if m in WIDE:
            continue
        for step in range(1, half):
            for i in range(2):
                from_mate(m, i, step).wait_recv()
                go(to_side(m, i, step))

    def weight_there(m):
        if m in WIDE:
            for step in range(1, half):
                from_mate(m, 0, step).wait_recv()
            return
        for step in range(half):
            for i in range(2):
                from_side(m, i, step).wait_recv()

    def weight(m):
        return wbuf[m].reshape(feats, cols)

    all_keys = lambda: kbuf[...].reshape(4 * tokens, feats)
    all_values = lambda: vbuf[...].reshape(4 * tokens, feats)

    def part_of(which):
        return pl.ds(pl.multiple_of(which * (cols // 2), cols // 2), cols // 2)

    def spread(s):
        column = turned(rbuf[s][0:1, :], tokens)
        return jnp.concatenate([column] * (cols // 2 // tokens), axis=1)

    def keep(m, s, which, value):
        lanes = pl.ds(pl.multiple_of(s * tokens, tokens), tokens)
        hid[m, part_of(which), lanes] = jnp.transpose(value).astype(jnp.bfloat16)

    def weigh(which):
        def one(s, carry):
            a_one, a_three = asum[ONE, s, :, part_of(which)], asum[THREE, s, :, part_of(which)]
            keep(TWO, s, which, -spread(s) * a_one * jax.nn.sigmoid(a_one) * a_three)
            return carry

        lax.fori_loop(0, 4, one, 0)

    line_bit = [bit_of(line, i) for i in range(line_bits)]
    starts = [jnp.int32(0)]
    for i in range(line_bits):
        starts.append(starts[-1] + line_bit[i] * (lines >> (i + 1)))
    pos = b * lines + starts[-1]

    def gradient(v, which):
        m = v // SPLIT
        ref = vbuf if m == TWO else kbuf
        side_rows = ref[:, :, lanes_of(v)].reshape(4 * tokens, wide)
        return dot(hid[m, part_of(which), :], side_rows).reshape(lines, unit, wide)

    def offset(step):
        return blocks - 2 * (lines >> step)

    def send_sum(m, step):
        at = pl.ds(offset(step), lines >> step)
        to = side if step == 0 else in_role(flipped(line, step - 1), a, b, core)
        return remote(
            staged.at[m, at], landed.at[m, at], sum_s.at[m, step], sum_r.at[m, step], to
        )

    def send_away(m):
        for v in parts(m):
            staged[v, pl.ds(0, lines)] = gradient(v, 1 - b).astype(jnp.bfloat16)
            go(send_sum(v, 0))

    def keep_own(m):
        for v in parts(m):
            total[v] = gradient(v, b)

    def keep_old(m):
        lanes = pl.ds(pl.multiple_of(b * (cols // 2), cols // 2), cols // 2)
        mine = wbuf[m, :, :, lanes].reshape(feats, cols // 2).astype(jnp.float32)
        old_all[...] = jnp.transpose(mine).reshape(lines, unit, feats)
        old_own[m] = old_all[starts[-1]]

    def deltas(which):
        def one(s, carry):
            a_one, a_three = asum[ONE, s, :, part_of(which)], asum[THREE, s, :, part_of(which)]
            back = -spread(s) * asum[TWO, s, :, part_of(which)]
            sig = jax.nn.sigmoid(a_one)
            keep(ONE, s, which, back * a_three * sig * (1.0 + a_one * (1.0 - sig)))
            keep(THREE, s, which, back * a_one * sig)
            return carry

        lax.fori_loop(0, 4, one, 0)

    seg_copy = remote(seg_ref, old_seg, halo_s.at[4], halo_r.at[4], after)
    kinds = ((k_ref, kbuf, old_k), (v_ref, vbuf, old_v))

    def upward(i):
        src = kinds[i][1].at[3]
        return remote(src, relay.at[i], up_s.at[i], up_r.at[i], around(8))

    def halo(i, group, relayed=False):
        ref, buf, old = kinds[i]
        if group is None:
            return remote(ref, old, halo_s.at[i], halo_r.at[i], partner)
        at = old.at[:, pl.ds(group * feats, feats)]
        if group == 0:
            slot, to = 3, device(line, 0, 1 - y, 0)
        else:
            slot, to = (y + x - 2 * x * y) * 2 + 1, device(line, 1 - x, y, 0)
        src = relay.at[i] if relayed else buf.at[slot]
        return remote(src, at, halo_s.at[i * 2 + group], halo_r.at[i * 2 + group], to)

    def halo_from(i, group):
        if group is None:
            return halo(i, None)
        at = kinds[i][2].at[:, pl.ds(group * feats, feats)]
        return remote(at, at, halo_s.at[i * 2 + group], halo_r.at[i * 2 + group], partner)

    edge_zero = (core == 0) & (x == 0) & (y == 1)
    edge_one = (core == 1) & (x == 1) & (y == 0)
    edge = edge_zero | edge_one
    plain_zero = (core == 0) & (x == 0) & (y == 0)
    plain_one = (core == 1) & jnp.logical_not(edge_one)

    def both(predicate, act):
        @pl.when(predicate)
        def _():
            for i in range(2):
                act(i)

    def halo_sends(act):
        both(core == 0, lambda i: act(halo(i, None)))
        both(plain_zero, lambda i: act(halo(i, 0)))
        both(plain_one, lambda i: act(halo(i, 1)))
        both(edge_zero & (line > 0), lambda i: act(halo(i, 0, True)))
        both(edge_one & (line > 0), lambda i: act(halo(i, 1, True)))

        @pl.when(me != count - 1)
        def _():
            act(seg_copy)

    def project(m):
        weight_there(m)
        rows_in = all_values() if m == TWO else all_keys()
        asum[m] = dot(rows_in, weight(m)).reshape(4, tokens, cols)

    take_tokens(0)
    take_tokens(3)
    project(ONE)
    project(THREE)
    weigh(1 - b)
    take_tokens(1)
    both(edge & (line < lines - 1), lambda i: upward(i).start())
    send_away(TWO)
    weigh(b)
    keep_own(TWO)
    keep_old(ONE)
    keep_old(THREE)
    project(TWO)
    deltas(1 - b)
    send_away(ONE)
    send_away(THREE)
    send_tokens(2)

    both(edge & (line > 0), lambda i: upward(i).wait_recv())
    halo_sends(lambda copy: copy.start())

    @pl.when(me == 0)
    def _():
        old_k[...] = jnp.zeros_like(old_k)
        old_v[...] = jnp.zeros_like(old_v)
        old_seg[...] = jnp.zeros_like(old_seg)

    @pl.when((core == 0) & (x == 1))
    def _():
        for _, buf, old in kinds:
            old[:, 0:feats] = buf[1]

    order = (TWO, ONE, THREE)

    def pass_on(m, step):
        size = lines >> step
        bit = line_bit[step - 1]
        kept, away = starts[step], starts[step - 1] + (1 - bit) * size
        shift = offset(step - 1) - starts[step - 1]
        send_sum(m, step - 1).wait_recv()

        def stage(i, carry):
            value = total[m, away + i] + landed[m, shift + away + i].astype(jnp.float32)
            staged[m, offset(step) + i] = value.astype(jnp.bfloat16)
            return carry

        def hold(i, carry):
            value = total[m, kept + i] + landed[m, shift + kept + i].astype(jnp.float32)
            total[m, kept + i] = value
            return carry

        lax.fori_loop(0, size, stage, 0)
        go(send_sum(m, step))
        lax.fori_loop(0, size, hold, 0)

    def pass_all(m, step):
        for v in parts(m):
            pass_on(v, step)

    def span(part, position):
        if part == 0:
            return pl.ds(position, 1)
        size = 1 << (part - 1)
        return pl.ds(flipped(lax.div(position, jnp.int32(size)), 0) * size, size)

    def send_new(m, step, part):
        src = new.at[m, 0, span(part, pos)]
        if step == steps:
            dst, to = new.at[m, 1, span(part, pos)], pair
        elif step == steps - 1:
            dst, to = src, side
        else:
            dst, to = src, in_role(flipped(line, line_bits - 1 - step), a, b, core)
        return remote(src, dst, all_s.at[m, step, part], all_r.at[m, step, part], to)

    def new_there(m, step, part):
        if step == steps:
            ref = new.at[m, 1, span(part, pos)]
        else:
            ref = new.at[m, 0, span(part, flipped(pos, step))]
        return remote(ref, ref, all_s.at[m, step, part], all_r.at[m, step, part], side)

    def last_step(v):
        return steps + 1 if v // SPLIT == TWO else steps

    def renew(m):
        updates, square = [], 0.0
        for v in parts(m):
            send_sum(v, steps - 1).wait_recv()
            grad = total[v, starts[-1]] + landed[v, offset(steps - 1)].astype(jnp.float32)
            updates.append(old_own[m, :, lanes_of(v)] - grad)
            square += jnp.sum(updates[-1] * updates[-1], axis=1, keepdims=True)
        old = old_own[m]
        old_len = jnp.sqrt(jnp.sum(old * old, axis=1, keepdims=True))
        ratio = old_len / jnp.sqrt(square + EPS)
        for v, update in zip(parts(m), updates):
            new[v, 0, pos] = (update * ratio).astype(jnp.bfloat16)
            for step in range(last_step(v)):
                go(send_new(v, step, 0))

    pass_all(TWO, 1)
    deltas(b)
    keep_own(ONE)
    pass_all(ONE, 1)
    keep_own(THREE)
    pass_all(THREE, 1)
    keep_old(TWO)
    for step in range(2, steps):
        for m in order:
            pass_all(m, step)
    for m in order:
        renew(m)

    dim = width // ATT_HEADS
    scale = 1.0 / math.sqrt(dim)

    both(core == 1, lambda i: halo_from(i, None).wait_recv())
    both((core == 0) & (x == 0) & (me != 0), lambda i: halo_from(i, 0).wait_recv())
    both((core == 0) & (me != 0), lambda i: halo_from(i, 1).wait_recv())

    @pl.when(me != 0)
    def _():
        seg_copy.wait_recv()

    def attend(first_head, last_head):
        row = lax.broadcasted_iota(jnp.int32, (tokens, tokens), 0)
        col = lax.broadcasted_iota(jnp.int32, (tokens, tokens), 1)
        seg_row = seg_ref[...].astype(jnp.float32)
        seg_col = turned(seg_row, tokens)
        now_ok = (col <= row) & (row - col < WINDOW) & (seg_col == seg_row)
        old_ok = (
            (row - col + tokens < WINDOW)
            & (seg_col == old_seg[...].astype(jnp.float32))
            & (row + me * tokens >= row + tokens)
        )

        def one(i, carry):
            lanes = pl.ds(pl.multiple_of(i * dim, dim), dim)
            q = q_ref[:, lanes]

            def score(keys, allowed):
                return jnp.where(allowed, nt_dot(q, keys) * scale, jnp.float32(-1e30))

            old, now = score(old_k[:, lanes], old_ok), score(k_ref[:, lanes], now_ok)
            top = jnp.maximum(
                jnp.max(old, axis=1, keepdims=True), jnp.max(now, axis=1, keepdims=True)
            )
            old = jnp.where(old_ok, jnp.exp(old - top), jnp.float32(0.0))
            now = jnp.where(now_ok, jnp.exp(now - top), jnp.float32(0.0))
            norm = jnp.sum(old, axis=1, keepdims=True) + jnp.sum(now, axis=1, keepdims=True)
            out = dot((old / norm).astype(jnp.bfloat16), old_v[:, lanes]) + dot(
                (now / norm).astype(jnp.bfloat16), v_ref[:, lanes]
            )
            att_ref[:, lanes] = out.astype(jnp.bfloat16)
            return carry

        lax.fori_loop(first_head, last_head, one, 0)

    def query_dot(m, rows_q):
        return sum(nt_dot(rows_q[:, lanes_of(v)], flat(new[v, 0])) for v in parts(m))

    def mixed(place_from):
        slots = pl.ds(place_from * 2, 2)
        b_one = asum[ONE, slots].reshape(2 * tokens, cols)
        b_three = query_dot(THREE, qbuf[slots].reshape(2 * tokens, feats))
        return (jax.nn.silu(b_one) * b_three).astype(jnp.bfloat16)

    turns = [(step, m, v) for step in range(steps) for m in order for v in parts(m)]
    slots = len(turns) - 2
    for slot, (step, m, v) in enumerate(turns):
        for part in range(step + 1):
            new_there(v, step, part).wait_recv()
        for later in range(step + 1, last_step(v)):
            go(send_new(v, later, step + 1))
        if slot < slots:
            attend(ATT_HEADS * slot // slots, ATT_HEADS * (slot + 1) // slots)
        if (step, v) == (steps - 1, parts(ONE)[-1]):
            take_tokens(2)
            rows_q = qbuf[...].reshape(4 * tokens, feats)
            asum[ONE] = query_dot(ONE, rows_q).reshape(4, tokens, cols)

    z_send[...] = mixed(1 - a)
    z_copy = remote(z_send, z_peer, end_s.at[0], end_r.at[0], pair)
    go(z_copy)
    z_own[...] = mixed(a)
    for v in parts(TWO):
        for part in range(steps + 1):
            new_there(v, steps, part).wait_recv()
    z_copy.wait_recv()

    def fast_rows(c, v):
        at = pl.ds(pl.multiple_of(c * tokens, tokens), tokens)
        value = dot(z_own[at, :], flat(new[v, 0])) + dot(z_peer[at, :], flat(new[v, 1]))
        return value.astype(jnp.bfloat16)

    for v in parts(TWO):
        o_send[:, lanes_of(v)] = fast_rows(other, v)
    out_copy = remote(
        o_send, out_ref.at[:, own_lanes(core)], end_s.at[1], end_r.at[1], partner
    )
    go(out_copy)
    for v in parts(TWO):
        lanes = pl.ds(pl.multiple_of(core * feats + v % SPLIT * wide, wide), wide)
        out_ref[:, lanes] = fast_rows(core, v)
    theirs = out_ref.at[:, own_lanes(other)]
    remote(theirs, theirs, end_s.at[1], end_r.at[1], partner).wait_recv()

    for copy in started:
        copy.wait_send()
    for m in range(3):

        @pl.when(core == head)
        def _():
            for i in range(pairs(m)):
                to_mirror(m, i).wait_send()

        @pl.when(core != head)
        def _():
            first(m, 0).wait_send()

    halo_sends(lambda copy: copy.wait_send())
    both(edge & (line < lines - 1), lambda i: upward(i).wait_send())


def per_device(queries, keys, values, segment, rates, fast_one, fast_three, fast_two):
    count = lax.axis_size("tok")
    tokens, width = queries.shape
    rows, hidden = fast_one.shape
    lines = count // 8
    half = lines // 2
    steps = lines.bit_length()
    feats = width // FAST_HEADS
    cols = hidden // 2
    blocks = 2 * lines
    unit = cols // blocks
    wide = feats // SPLIT
    bf16, f32 = jnp.bfloat16, jnp.float32
    dma = pltpu.SemaphoreType.DMA
    operands = (
        fast_one, fast_three, fast_two, queries, keys, values, segment.reshape(1, tokens), rates.T
    )
    return pl.pallas_call(
        functools.partial(kernel, count),
        out_shape=[jax.ShapeDtypeStruct(queries.shape, bf16)] * 2,
        in_specs=[pl.BlockSpec(memory_space=pltpu.HBM)] * 8,
        out_specs=[pl.BlockSpec(memory_space=pltpu.VMEM)] * 2,
        scratch_shapes=[pltpu.VMEM(one.shape, one.dtype) for one in operands]
        + [
            dma((8,)),
            pltpu.VMEM((3, count // 4, 2 * rows, cols), bf16),
            pltpu.VMEM((4, tokens, feats), bf16),
            pltpu.VMEM((4, tokens, feats), bf16),
            pltpu.VMEM((4, tokens, feats), bf16),
            pltpu.VMEM((4, 8, tokens), f32),
            pltpu.VMEM((FAST_HEADS, 8, tokens), f32),
            pltpu.VMEM((3, 4, tokens, cols), f32),
            pltpu.VMEM((3, cols, 4 * tokens), bf16),
            pltpu.VMEM((3 * SPLIT, lines, unit, wide), f32),
            pltpu.VMEM((3 * SPLIT, blocks, unit, wide), bf16),
            pltpu.VMEM((3 * SPLIT, blocks, unit, wide), bf16),
            pltpu.VMEM((3, unit, feats), f32),
            pltpu.VMEM((lines, unit, feats), f32),
            pltpu.VMEM((3 * SPLIT, 2, blocks, unit, wide), bf16),
            pltpu.VMEM((2 * tokens, cols), bf16),
            pltpu.VMEM((2 * tokens, cols), bf16),
            pltpu.VMEM((2 * tokens, cols), bf16),
            pltpu.VMEM((tokens, feats), bf16),
            pltpu.VMEM(keys.shape, bf16),
            pltpu.VMEM(values.shape, bf16),
            pltpu.VMEM((1, tokens), jnp.int32),
            pltpu.VMEM((2, tokens, feats), bf16),
            dma((3, 4)),
            dma((3, 4, 2)),
            dma((3,)),
            dma((3, 2)),
            dma((3, 2)),
            dma((3, 2, half)),
            dma((3, 2, half)),
            dma((3, 2, half)),
            dma((3, 2, half)),
            dma((4, 3)),
            dma((4, 3)),
            dma((3 * SPLIT, steps)),
            dma((3 * SPLIT, steps)),
            dma((3 * SPLIT, steps + 1, steps + 1)),
            dma((3 * SPLIT, steps + 1, steps + 1)),
            dma((2,)),
            dma((2,)),
            dma((5,)),
            dma((5,)),
            dma((2,)),
            dma((2,)),
        ],
        compiler_params=pltpu.CompilerParams(
            collective_id=0, has_side_effects=True, vmem_limit_bytes=40 << 20
        ),
    )(*[pltpu.with_memory_space_constraint(one, pltpu.HBM) for one in operands])


def solution(mesh):
    placed = P(("grp", "tok"), None)
    return jax.shard_map(
        per_device,
        mesh=mesh,
        in_specs=(placed, placed, placed, P(("grp", "tok")), placed, placed, placed, placed),
        out_specs=(placed, placed),
        check_vma=False,
    )
```

```python
import functools
import math

import jax
import jax.numpy as jnp
from jax import lax
from jax.experimental import pallas as pl
from jax.experimental.pallas import tpu as pltpu
from jax.sharding import PartitionSpec as P

ATT_HEADS = 16
FAST_HEADS = 2
WINDOW = 128
EPS = 1e-06

ONE, THREE, TWO = 0, 1, 2
WIDE = (TWO,)
SPLIT = 2
PAIR = -1


def device(line, x, y, core):
    return ((line * 2 + y) * 2 + x) * 2 + core


def in_role(line, a, b, role):
    return device(line, a + role * (b - a), b + role * (a - b), role)


def bit_of(index, bit):
    return lax.rem(lax.div(index, jnp.int32(1 << bit)), jnp.int32(2))


def flipped(index, bit):
    return index + (1 - 2 * bit_of(index, bit)) * (1 << bit)


def remote(src, dst, send_sem, recv_sem, partner):
    return pltpu.make_async_remote_copy(
        src_ref=src,
        dst_ref=dst,
        send_sem=send_sem,
        recv_sem=recv_sem,
        device_id={"tok": partner},
        device_id_type=pl.DeviceIdType.MESH,
    )


def turned(row, size):
    return jnp.transpose(jnp.broadcast_to(row, (size, size)))


def nt_dot(left, right):
    return lax.dot_general(
        left, right, (((1,), (1,)), ((), ())), preferred_element_type=jnp.float32
    )


def dot(left, right):
    return jnp.dot(left, right, preferred_element_type=jnp.float32)


def flat(blocks):
    n, unit, width = blocks.shape
    if unit % 16 == 0:
        return blocks.reshape(n * unit, width)
    return blocks.astype(jnp.float32).reshape(n * unit, width).astype(jnp.bfloat16)


def merged(regions):
    regions = sorted((which, offs // size * size, size) for which, offs, size in regions)
    for which, offs, size in regions:
        twin = (which, offs ^ size, size)
        if twin in regions:
            rest = [one for one in regions if one not in ((which, offs, size), twin)]
            return merged(rest + [(which, min(offs, offs ^ size), 2 * size)])
    return regions


def spread_plan(steps, moved):
    groups, plan = [[(0, 0, 1)]], []
    for step in steps:
        known = [(group, region) for group, held in enumerate(groups) for region in held]
        plan.append([((group, i), region) for i, (group, region) in enumerate(known)])
        groups.append(merged([moved(region, step) for _, region in known]))
    return plan


def kernel(count, *refs):
    att_ref, out_ref = refs[8:10]
    loaded, load_sem = refs[10:18], refs[18]
    w_refs = loaded[:3]
    q_ref, k_ref, v_ref, seg_ref, rate_ref = loaded[3:8]
    (
        wbuf, kbuf, vbuf, qbuf, rbuf, rsend, asum, hid, total, staged, landed, old_own, old_all, new,
        z_own, z_peer, z_send, o_send, old_k, old_v, old_seg, relay,
        first_s, first_r, first_l, mirror_s, mirror_r, mate_s, mate_r, side_s, side_r,
        tok_s, tok_r, sum_s, sum_r, all_s, all_r, end_s, end_r, halo_s, halo_r, up_s, up_r,
    ) = refs[19:]

    lines = count // 8
    half = lines // 2
    line_bits = lines.bit_length() - 1
    steps = line_bits + 1
    rows, hidden = w_refs[0].shape
    cols = hidden // 2
    tokens, width = q_ref.shape
    feats = width // FAST_HEADS
    blocks = 2 * lines
    unit = cols // blocks
    wide = feats // SPLIT

    def parts(m):
        return range(m * SPLIT, (m + 1) * SPLIT)

    def lanes_of(v):
        return slice(v % SPLIT * wide, (v % SPLIT + 1) * wide)

    me = lax.axis_index("tok")
    core, chip = lax.rem(me, 2), lax.div(me, 2)
    x, y, line = lax.rem(chip, 2), lax.rem(lax.div(chip, 2), 2), lax.div(chip, 4)
    a, b = x + core * (y - x), y + core * (x - y)
    a_other, b_other = b, a
    other = 1 - core
    partner = device(line, x, y, other)
    pair = in_role(line, 1 - a, b, core)
    side = in_role(line, a, 1 - b, core)
    pair_takes = in_role(line, 1 - a_other, b_other, other)
    mirror_line = lax.rem(line + half, lines)
    mirror = in_role(mirror_line, a, b, core)
    upper = lax.div(line, half)
    place = line - upper * half
    base = upper * half

    def mate(i):
        return in_role(base + lax.rem(place + i, half), a, b, core)

    def around(i):
        return lax.rem(me + count + i, count)

    after = around(1)
    loads = [pltpu.make_async_copy(refs[i], loaded[i], load_sem.at[i]) for i in range(8)]
    loading = (0, 1, 2, 4, 7, 5, 6, 3)
    for i in loading:
        loads[i].start()

    barrier = pltpu.get_barrier_semaphore()
    plane = line * 8
    known = [plane + lax.rem(me - plane + i, 8) for i in range(1, 8)]
    known += [mirror] + [mate(i) for i in range(1, half)]
    known += [around(i) for i in (1, -1, 8, -8)]
    for one in known:
        pl.semaphore_signal(
            barrier, inc=1, device_id={"tok": one}, device_id_type=pl.DeviceIdType.MESH
        )
    for i in loading:
        loads[i].wait()
    for group in range(FAST_HEADS):
        rsend[group] = jnp.broadcast_to(rate_ref[group : group + 1, :], (8, tokens))
    pl.semaphore_wait(barrier, len(known))

    started = []

    def go(copy):
        copy.start()
        started.append(copy)

    head = upper
    head_a, head_b = x + head * (y - x), y + head * (x - y)
    stored = place * 4 + y * 2 + x

    def first(m, far):
        cross, apart = far % 2, far // 2
        start = (head_a + cross - 2 * cross * head_a) * cols
        src = w_refs[m].at[:, pl.ds(pl.multiple_of(start, cols), cols)]
        dst = wbuf.at[m, stored, pl.ds(pl.multiple_of(core * rows, rows), rows), :]
        to_a = 1 - head_a if cross else head_a
        to = in_role(line, to_a, 1 - head_b if apart else head_b, head)
        return remote(src, dst, first_s.at[m, far], first_r.at[m, far, core], to)

    def first_here(m):
        src = w_refs[m].at[:, pl.ds(pl.multiple_of(head_a * cols, cols), cols)]
        dst = wbuf.at[m, stored, pl.ds(pl.multiple_of(core * rows, rows), rows), :]
        return pltpu.make_async_copy(src, dst, first_l.at[m])

    def reach(m):
        return 4 if m in WIDE else 2

    for m in range(3):
        for far in range(1, reach(m)):
            go(first(m, far))

        @pl.when(core == head)
        def _():
            first_here(m).start()

        @pl.when(core != head)
        def _():
            first(m, 0).start()

    def own_lanes(group):
        return pl.ds(pl.multiple_of(group * feats, feats), feats)

    def send_tokens(kind):
        ref, buf = ((k_ref, kbuf), (v_ref, vbuf), (q_ref, qbuf), (rsend, rbuf))[kind]
        if kind == 3:
            mine, theirs = ref.at[core], ref.at[other]
        else:
            mine, theirs = ref.at[:, own_lanes(core)], ref.at[:, own_lanes(other)]
        here, there = buf.at[a * 2 + core], buf.at[a_other * 2 + core]
        go(remote(mine, here, tok_s.at[kind, 0], tok_r.at[kind, 1 + core], pair))
        go(remote(theirs, there, tok_s.at[kind, 1], tok_r.at[kind, 0], partner))
        go(remote(theirs, there, tok_s.at[kind, 2], tok_r.at[kind, 1 + core], pair_takes))
        if kind == 3:
            rbuf[a * 2 + core] = rsend[core]
        else:
            buf[a * 2 + core] = ref[:, own_lanes(core)]

    def take_tokens(kind):
        buf = (kbuf, vbuf, qbuf, rbuf)[kind]
        for i, slot in ((0, a * 2 + other), (1, (1 - a) * 2), (2, (1 - a) * 2 + 1)):
            ref = buf.at[slot]
            remote(ref, ref, tok_s.at[kind, i], tok_r.at[kind, i], partner).wait_recv()

    send_tokens(0)
    send_tokens(3)
    send_tokens(1)

    def pairs(m):
        return 1 if m in WIDE else 2

    def piece(m, k, i, b_from):
        if m in WIDE:
            return wbuf.at[m, pl.ds(k * 4, 4)]
        return wbuf.at[m, k * 4 + b_from * 2 + i + core * (i - b_from)]

    def first_wait(m):
        first_here(m).wait()
        for far in range(reach(m)):
            from_a = 1 - a if far % 2 else a
            from_b = 1 - b if far // 2 else b
            block = wbuf.at[m, place * 4 + from_b * 2 + from_a + core * (from_a - from_b)]
            for c in (other,) if far == 0 else (0, 1):
                ref = block.at[pl.ds(pl.multiple_of(c * rows, rows), rows), :]
                copy = remote(ref, ref, first_s.at[m, far], first_r.at[m, far, c], partner)
                copy.wait_recv()

    def to_mirror(m, i):
        ref = piece(m, place, i, b)
        return remote(ref, ref, mirror_s.at[m, i], mirror_r.at[m, i], mirror)

    def to_mate(m, i, step):
        ref = piece(m, place, i, b)
        return remote(ref, ref, mate_s.at[m, i, step], mate_r.at[m, i, step], mate(step))

    def from_mate(m, i, step):
        ref = piece(m, lax.rem(place + half - step, half), i, b)
        return remote(ref, ref, mate_s.at[m, i, step], mate_r.at[m, i, step], mate(step))

    def to_side(m, i, step):
        ref = piece(m, lax.rem(place + half - step, half), i, b)
        return remote(ref, ref, side_s.at[m, i, step], side_r.at[m, i, step], side)

    def from_side(m, i, step):
        ref = piece(m, lax.rem(place + half - step, half), i, 1 - b)
        return remote(ref, ref, side_s.at[m, i, step], side_r.at[m, i, step], side)

    for m in range(3):

        @pl.when(core == head)
        def _():
            first_wait(m)
            for i in range(pairs(m)):
                to_mirror(m, i).start()

        @pl.when(core != head)
        def _():
            for i in range(pairs(m)):
                to_mirror(m, i).wait_recv()

        for i in range(pairs(m)):
            for step in range(1, half):
                go(to_mate(m, i, step))
            if m not in WIDE:
                go(to_side(m, i, 0))
    for m in range(3):
        if m in WIDE:
            continue
        for step in range(1, half):
            for i in range(2):
                from_mate(m, i, step).wait_recv()
                go(to_side(m, i, step))

    def weight_there(m):
        if m in WIDE:
            for step in range(1, half):
                from_mate(m, 0, step).wait_recv()
            return
        for step in range(half):
            for i in range(2):
                from_side(m, i, step).wait_recv()

    def weight(m):
        return wbuf[m].reshape(feats, cols)

    all_keys = lambda: kbuf[...].reshape(4 * tokens, feats)
    all_values = lambda: vbuf[...].reshape(4 * tokens, feats)

    def part_of(which):
        return pl.ds(pl.multiple_of(which * (cols // 2), cols // 2), cols // 2)

    def spread(s):
        column = turned(rbuf[s][0:1, :], tokens)
        return jnp.concatenate([column] * (cols // 2 // tokens), axis=1)

    def keep(m, s, which, value):
        lanes = pl.ds(pl.multiple_of(s * tokens, tokens), tokens)
        hid[m, part_of(which), lanes] = jnp.transpose(value).astype(jnp.bfloat16)

    def weigh(which):
        def one(s, carry):
            a_one, a_three = asum[ONE, s, :, part_of(which)], asum[THREE, s, :, part_of(which)]
            keep(TWO, s, which, -spread(s) * a_one * jax.nn.sigmoid(a_one) * a_three)
            return carry

        lax.fori_loop(0, 4, one, 0)

    line_bit = [bit_of(line, i) for i in range(line_bits)]
    starts = [jnp.int32(0)]
    for i in range(line_bits):
        starts.append(starts[-1] + line_bit[i] * (lines >> (i + 1)))
    pos = b * lines + starts[-1]

    def gradient(v, which):
        m = v // SPLIT
        ref = vbuf if m == TWO else kbuf
        side_rows = ref[:, :, lanes_of(v)].reshape(4 * tokens, wide)
        return dot(hid[m, part_of(which), :], side_rows).reshape(lines, unit, wide)

    def offset(step):
        return blocks - 2 * (lines >> step)

    def send_sum(m, step):
        at = pl.ds(offset(step), lines >> step)
        to = side if step == 0 else in_role(flipped(line, step - 1), a, b, core)
        return remote(
            staged.at[m, at], landed.at[m, at], sum_s.at[m, step], sum_r.at[m, step], to
        )

    def send_away(m):
        for v in parts(m):
            staged[v, pl.ds(0, lines)] = gradient(v, 1 - b).astype(jnp.bfloat16)
            go(send_sum(v, 0))

    def keep_own(m):
        for v in parts(m):
            total[v] = gradient(v, b)

    def keep_old(m):
        lanes = pl.ds(pl.multiple_of(b * (cols // 2), cols // 2), cols // 2)
        mine = wbuf[m, :, :, lanes].reshape(feats, cols // 2).astype(jnp.float32)
        old_all[...] = jnp.transpose(mine).reshape(lines, unit, feats)
        old_own[m] = old_all[starts[-1]]

    def deltas(which):
        def one(s, carry):
            a_one, a_three = asum[ONE, s, :, part_of(which)], asum[THREE, s, :, part_of(which)]
            back = -spread(s) * asum[TWO, s, :, part_of(which)]
            sig = jax.nn.sigmoid(a_one)
            keep(ONE, s, which, back * a_three * sig * (1.0 + a_one * (1.0 - sig)))
            keep(THREE, s, which, back * a_one * sig)
            return carry

        lax.fori_loop(0, 4, one, 0)

    order = (TWO, ONE, THREE)

    def pass_on(m, step):
        size = lines >> step
        bit = line_bit[step - 1]
        kept, away = starts[step], starts[step - 1] + (1 - bit) * size
        shift = offset(step - 1) - starts[step - 1]
        send_sum(m, step - 1).wait_recv()

        def stage(i, carry):
            value = total[m, away + i] + landed[m, shift + away + i].astype(jnp.float32)
            staged[m, offset(step) + i] = value.astype(jnp.bfloat16)
            return carry

        def hold(i, carry):
            value = total[m, kept + i] + landed[m, shift + kept + i].astype(jnp.float32)
            total[m, kept + i] = value
            return carry

        lax.fori_loop(0, size, stage, 0)
        go(send_sum(m, step))
        lax.fori_loop(0, size, hold, 0)

    def pass_all(m, step):
        for v in parts(m):
            pass_on(v, step)

    seg_copy = remote(seg_ref, old_seg, halo_s.at[4], halo_r.at[4], after)
    kinds = ((k_ref, kbuf, old_k), (v_ref, vbuf, old_v))

    def upward(i):
        src = kinds[i][1].at[3]
        return remote(src, relay.at[i], up_s.at[i], up_r.at[i], around(8))

    def halo(i, group, relayed=False):
        ref, buf, old = kinds[i]
        if group is None:
            return remote(ref, old, halo_s.at[i], halo_r.at[i], partner)
        at = old.at[:, pl.ds(group * feats, feats)]
        if group == 0:
            slot, to = 3, device(line, 0, 1 - y, 0)
        else:
            slot, to = (y + x - 2 * x * y) * 2 + 1, device(line, 1 - x, y, 0)
        src = relay.at[i] if relayed else buf.at[slot]
        return remote(src, at, halo_s.at[i * 2 + group], halo_r.at[i * 2 + group], to)

    def halo_from(i, group):
        if group is None:
            return halo(i, None)
        at = kinds[i][2].at[:, pl.ds(group * feats, feats)]
        return remote(at, at, halo_s.at[i * 2 + group], halo_r.at[i * 2 + group], partner)

    edge_zero = (core == 0) & (x == 0) & (y == 1)
    edge_one = (core == 1) & (x == 1) & (y == 0)
    edge = edge_zero | edge_one
    plain_zero = (core == 0) & (x == 0) & (y == 0)
    plain_one = (core == 1) & jnp.logical_not(edge_one)

    def both(predicate, act):
        @pl.when(predicate)
        def _():
            for i in range(2):
                act(i)

    def halo_sends(act):
        both(core == 0, lambda i: act(halo(i, None)))
        both(plain_zero, lambda i: act(halo(i, 0)))
        both(plain_one, lambda i: act(halo(i, 1)))
        both(edge_zero & (line > 0), lambda i: act(halo(i, 0, True)))
        both(edge_one & (line > 0), lambda i: act(halo(i, 1, True)))

        @pl.when(me != count - 1)
        def _():
            act(seg_copy)

    def project(m):
        weight_there(m)
        rows_in = all_values() if m == TWO else all_keys()
        asum[m] = dot(rows_in, weight(m)).reshape(4, tokens, cols)

    take_tokens(0)
    take_tokens(3)
    project(ONE)
    project(THREE)
    weigh(1 - b)
    take_tokens(1)
    both(edge & (line < lines - 1), lambda i: upward(i).start())
    send_away(TWO)
    weigh(b)
    keep_own(TWO)
    keep_old(ONE)
    keep_old(THREE)
    project(TWO)
    deltas(1 - b)
    send_away(ONE)
    pass_all(TWO, 1)
    send_away(THREE)
    send_tokens(2)

    both(edge & (line > 0), lambda i: upward(i).wait_recv())
    halo_sends(lambda copy: copy.start())

    @pl.when(me == 0)
    def _():
        old_k[...] = jnp.zeros_like(old_k)
        old_v[...] = jnp.zeros_like(old_v)
        old_seg[...] = jnp.zeros_like(old_seg)

    @pl.when((core == 0) & (x == 1))
    def _():
        for _, buf, old in kinds:
            old[:, 0:feats] = buf[1]

    pos_bits = line_bit[::-1] + [b]
    low = list(range(line_bits - 1))
    orders = {
        ONE: low + [line_bits - 1, line_bits],
        THREE: low + [line_bits - 1, line_bits],
        TWO: low + [PAIR, line_bits - 1, line_bits],
    }

    def moved(region, step):
        which, offs, size = region
        return (1 - which, offs, size) if step == PAIR else (which, offs ^ (1 << step), size)

    plans = {m: spread_plan(orders[m], moved) for m in order}

    def block_of(v, region):
        which, offs, size = region
        start = jnp.int32(0)
        for i, bit in enumerate(pos_bits):
            if (1 << i) >= size:
                start += (1 - bit if (offs >> i) & 1 else bit) * (1 << i)
        return new.at[v, which, pl.ds(start, size)]

    def partner_at(step):
        if step == PAIR:
            return pair
        if step == line_bits:
            return side
        return in_role(flipped(line, line_bits - 1 - step), a, b, core)

    def new_copy(v, turn, index, src, dst):
        to = partner_at(orders[v // SPLIT][turn])
        return remote(src, dst, all_s.at[v, turn, index], all_r.at[v, turn, index], to)

    def send_group(v, group):
        m = v // SPLIT
        for turn in range(group, len(orders[m])):
            for index, region in plans[m][turn]:
                if index[0] != group:
                    continue
                dst = region if orders[m][turn] != PAIR else (1 - region[0],) + region[1:]
                go(new_copy(v, turn, index[1], block_of(v, region), block_of(v, dst)))

    def new_wait(v, turn):
        m = v // SPLIT
        for index, region in plans[m][turn]:
            ref = block_of(v, moved(region, orders[m][turn]))
            new_copy(v, turn, index[1], ref, ref).wait_recv()

    def renew(m):
        updates, square = [], 0.0
        for v in parts(m):
            send_sum(v, steps - 1).wait_recv()
            grad = total[v, starts[-1]] + landed[v, offset(steps - 1)].astype(jnp.float32)
            updates.append(old_own[m, :, lanes_of(v)] - grad)
            square += jnp.sum(updates[-1] * updates[-1], axis=1, keepdims=True)
        old = old_own[m]
        old_len = jnp.sqrt(jnp.sum(old * old, axis=1, keepdims=True))
        ratio = old_len / jnp.sqrt(square + EPS)
        for v, update in zip(parts(m), updates):
            new[v, 0, pos] = (update * ratio).astype(jnp.bfloat16)
            send_group(v, 0)

    deltas(b)
    keep_own(ONE)
    pass_all(ONE, 1)
    keep_own(THREE)
    pass_all(THREE, 1)
    keep_old(TWO)
    for step in range(2, steps):
        for m in order:
            pass_all(m, step)
    for m in order:
        renew(m)

    dim = width // ATT_HEADS
    scale = 1.0 / math.sqrt(dim)

    both(core == 1, lambda i: halo_from(i, None).wait_recv())
    both((core == 0) & (x == 0) & (me != 0), lambda i: halo_from(i, 0).wait_recv())
    both((core == 0) & (me != 0), lambda i: halo_from(i, 1).wait_recv())

    @pl.when(me != 0)
    def _():
        seg_copy.wait_recv()

    def attend(first_head, last_head):
        row = lax.broadcasted_iota(jnp.int32, (tokens, tokens), 0)
        col = lax.broadcasted_iota(jnp.int32, (tokens, tokens), 1)
        seg_row = seg_ref[...].astype(jnp.float32)
        seg_col = turned(seg_row, tokens)
        now_ok = (col <= row) & (row - col < WINDOW) & (seg_col == seg_row)
        old_ok = (
            (row - col + tokens < WINDOW)
            & (seg_col == old_seg[...].astype(jnp.float32))
            & (row + me * tokens >= row + tokens)
        )

        def one(i, carry):
            lanes = pl.ds(pl.multiple_of(i * dim, dim), dim)
            q = q_ref[:, lanes]

            def score(keys, allowed):
                return jnp.where(allowed, nt_dot(q, keys) * scale, jnp.float32(-1e30))

            old, now = score(old_k[:, lanes], old_ok), score(k_ref[:, lanes], now_ok)
            top = jnp.maximum(
                jnp.max(old, axis=1, keepdims=True), jnp.max(now, axis=1, keepdims=True)
            )
            old = jnp.where(old_ok, jnp.exp(old - top), jnp.float32(0.0))
            now = jnp.where(now_ok, jnp.exp(now - top), jnp.float32(0.0))
            norm = jnp.sum(old, axis=1, keepdims=True) + jnp.sum(now, axis=1, keepdims=True)
            out = dot((old / norm).astype(jnp.bfloat16), old_v[:, lanes]) + dot(
                (now / norm).astype(jnp.bfloat16), v_ref[:, lanes]
            )
            att_ref[:, lanes] = out.astype(jnp.bfloat16)
            return carry

        lax.fori_loop(first_head, last_head, one, 0)

    def query_dot(m, rows_q):
        return sum(nt_dot(rows_q[:, lanes_of(v)], flat(new[v, 0])) for v in parts(m))

    def mixed(place_from):
        slots = pl.ds(place_from * 2, 2)
        b_one = asum[ONE, slots].reshape(2 * tokens, cols)
        b_three = query_dot(THREE, qbuf[slots].reshape(2 * tokens, feats))
        return (jax.nn.silu(b_one) * b_three).astype(jnp.bfloat16)

    turns = [
        (turn, v)
        for turn in range(steps + 1)
        for m in order
        for v in parts(m)
        if turn < len(orders[m]) and turn < steps
    ]
    slots = len(turns) - 2
    for slot, (turn, v) in enumerate(turns):
        new_wait(v, turn)
        send_group(v, turn + 1)
        if slot < slots:
            attend(ATT_HEADS * slot // slots, ATT_HEADS * (slot + 1) // slots)
        if (turn, v) == (steps - 1, parts(ONE)[-1]):
            take_tokens(2)
            rows_q = qbuf[...].reshape(4 * tokens, feats)
            asum[ONE] = query_dot(ONE, rows_q).reshape(4, tokens, cols)

    z_send[...] = mixed(1 - a)
    z_copy = remote(z_send, z_peer, end_s.at[0], end_r.at[0], pair)
    go(z_copy)
    z_own[...] = mixed(a)
    for v in parts(TWO):
        new_wait(v, steps)
    z_copy.wait_recv()

    def fast_rows(c, v):
        at = pl.ds(pl.multiple_of(c * tokens, tokens), tokens)
        value = dot(z_own[at, :], flat(new[v, 0])) + dot(z_peer[at, :], flat(new[v, 1]))
        return value.astype(jnp.bfloat16)

    for v in parts(TWO):
        o_send[:, lanes_of(v)] = fast_rows(other, v)
    out_copy = remote(
        o_send, out_ref.at[:, own_lanes(core)], end_s.at[1], end_r.at[1], partner
    )
    go(out_copy)
    for v in parts(TWO):
        lanes = pl.ds(pl.multiple_of(core * feats + v % SPLIT * wide, wide), wide)
        out_ref[:, lanes] = fast_rows(core, v)
    theirs = out_ref.at[:, own_lanes(other)]
    remote(theirs, theirs, end_s.at[1], end_r.at[1], partner).wait_recv()

    for copy in started:
        copy.wait_send()
    for m in range(3):

        @pl.when(core == head)
        def _():
            for i in range(pairs(m)):
                to_mirror(m, i).wait_send()

        @pl.when(core != head)
        def _():
            first(m, 0).wait_send()

    halo_sends(lambda copy: copy.wait_send())
    both(edge & (line < lines - 1), lambda i: upward(i).wait_send())


def per_device(queries, keys, values, segment, rates, fast_one, fast_three, fast_two):
    count = lax.axis_size("tok")
    tokens, width = queries.shape
    rows, hidden = fast_one.shape
    lines = count // 8
    half = lines // 2
    steps = lines.bit_length()
    feats = width // FAST_HEADS
    cols = hidden // 2
    blocks = 2 * lines
    unit = cols // blocks
    wide = feats // SPLIT
    bf16, f32 = jnp.bfloat16, jnp.float32
    dma = pltpu.SemaphoreType.DMA
    operands = (
        fast_one, fast_three, fast_two, queries, keys, values, segment.reshape(1, tokens), rates.T
    )
    return pl.pallas_call(
        functools.partial(kernel, count),
        out_shape=[jax.ShapeDtypeStruct(queries.shape, bf16)] * 2,
        in_specs=[pl.BlockSpec(memory_space=pltpu.HBM)] * 8,
        out_specs=[pl.BlockSpec(memory_space=pltpu.VMEM)] * 2,
        scratch_shapes=[pltpu.VMEM(one.shape, one.dtype) for one in operands]
        + [
            dma((8,)),
            pltpu.VMEM((3, count // 4, 2 * rows, cols), bf16),
            pltpu.VMEM((4, tokens, feats), bf16),
            pltpu.VMEM((4, tokens, feats), bf16),
            pltpu.VMEM((4, tokens, feats), bf16),
            pltpu.VMEM((4, 8, tokens), f32),
            pltpu.VMEM((FAST_HEADS, 8, tokens), f32),
            pltpu.VMEM((3, 4, tokens, cols), f32),
            pltpu.VMEM((3, cols, 4 * tokens), bf16),
            pltpu.VMEM((3 * SPLIT, lines, unit, wide), f32),
            pltpu.VMEM((3 * SPLIT, blocks, unit, wide), bf16),
            pltpu.VMEM((3 * SPLIT, blocks, unit, wide), bf16),
            pltpu.VMEM((3, unit, feats), f32),
            pltpu.VMEM((lines, unit, feats), f32),
            pltpu.VMEM((3 * SPLIT, 2, blocks, unit, wide), bf16),
            pltpu.VMEM((2 * tokens, cols), bf16),
            pltpu.VMEM((2 * tokens, cols), bf16),
            pltpu.VMEM((2 * tokens, cols), bf16),
            pltpu.VMEM((tokens, feats), bf16),
            pltpu.VMEM(keys.shape, bf16),
            pltpu.VMEM(values.shape, bf16),
            pltpu.VMEM((1, tokens), jnp.int32),
            pltpu.VMEM((2, tokens, feats), bf16),
            dma((3, 4)),
            dma((3, 4, 2)),
            dma((3,)),
            dma((3, 2)),
            dma((3, 2)),
            dma((3, 2, half)),
            dma((3, 2, half)),
            dma((3, 2, half)),
            dma((3, 2, half)),
            dma((4, 3)),
            dma((4, 3)),
            dma((3 * SPLIT, steps)),
            dma((3 * SPLIT, steps)),
            dma((3 * SPLIT, steps + 1, 2 * steps)),
            dma((3 * SPLIT, steps + 1, 2 * steps)),
            dma((2,)),
            dma((2,)),
            dma((5,)),
            dma((5,)),
            dma((2,)),
            dma((2,)),
        ],
        compiler_params=pltpu.CompilerParams(
            collective_id=0, has_side_effects=True, vmem_limit_bytes=40 << 20
        ),
    )(*[pltpu.with_memory_space_constraint(one, pltpu.HBM) for one in operands])


def solution(mesh):
    placed = P(("grp", "tok"), None)
    return jax.shard_map(
        per_device,
        mesh=mesh,
        in_specs=(placed, placed, placed, P(("grp", "tok")), placed, placed, placed, placed),
        out_specs=(placed, placed),
        check_vma=False,
    )
```

```python
import functools
import math

import jax
import jax.numpy as jnp
from jax import lax
from jax.experimental import pallas as pl
from jax.experimental.pallas import tpu as pltpu
from jax.sharding import PartitionSpec as P

ATT_HEADS = 16
FAST_HEADS = 2
WINDOW = 128
EPS = 1e-06

ONE, THREE, TWO = 0, 1, 2
WIDE = (TWO,)
SPLIT = 2
PAIR = -1


def device(line, x, y, core):
    return ((line * 2 + y) * 2 + x) * 2 + core


def in_role(line, a, b, role):
    return device(line, a + role * (b - a), b + role * (a - b), role)


def bit_of(index, bit):
    return lax.rem(lax.div(index, jnp.int32(1 << bit)), jnp.int32(2))


def flipped(index, bit):
    return index + (1 - 2 * bit_of(index, bit)) * (1 << bit)


def remote(src, dst, send_sem, recv_sem, partner):
    return pltpu.make_async_remote_copy(
        src_ref=src,
        dst_ref=dst,
        send_sem=send_sem,
        recv_sem=recv_sem,
        device_id={"tok": partner},
        device_id_type=pl.DeviceIdType.MESH,
    )


def turned(row, size):
    return jnp.transpose(jnp.broadcast_to(row, (size, size)))


def nt_dot(left, right):
    return lax.dot_general(
        left, right, (((1,), (1,)), ((), ())), preferred_element_type=jnp.float32
    )


def dot(left, right):
    return jnp.dot(left, right, preferred_element_type=jnp.float32)


def flat(blocks):
    n, unit, width = blocks.shape
    if unit % 16 == 0:
        return blocks.reshape(n * unit, width)
    return blocks.astype(jnp.float32).reshape(n * unit, width).astype(jnp.bfloat16)


def merged(regions):
    regions = sorted((which, offs // size * size, size) for which, offs, size in regions)
    for which, offs, size in regions:
        twin = (which, offs ^ size, size)
        if twin in regions:
            rest = [one for one in regions if one not in ((which, offs, size), twin)]
            return merged(rest + [(which, min(offs, offs ^ size), 2 * size)])
    return regions


def spread_plan(steps, moved):
    groups, plan = [[(0, 0, 1)]], []
    for step in steps:
        known = [(group, region) for group, held in enumerate(groups) for region in held]
        plan.append([((group, i), region) for i, (group, region) in enumerate(known)])
        groups.append(merged([moved(region, step) for _, region in known]))
    return plan


def kernel(count, *refs):
    att_ref, out_ref = refs[8:10]
    loaded, load_sem = refs[10:18], refs[18]
    w_refs = loaded[:3]
    q_ref, k_ref, v_ref, seg_ref, rate_ref = loaded[3:8]
    (
        wbuf, kbuf, vbuf, qbuf, rbuf, rsend, asum, hid, total, staged, landed, old_own, old_all, new,
        z_own, z_peer, z_send, o_send, old_k, old_v, old_seg, relay,
        first_s, first_r, first_l, mirror_s, mirror_r, mate_s, mate_r, side_s, side_r,
        tok_s, tok_r, sum_s, sum_r, all_s, all_r, end_s, end_r, halo_s, halo_r, up_s, up_r,
    ) = refs[19:]

    lines = count // 8
    half = lines // 2
    line_bits = lines.bit_length() - 1
    steps = line_bits + 1
    rows, hidden = w_refs[0].shape
    cols = hidden // 2
    tokens, width = q_ref.shape
    feats = width // FAST_HEADS
    blocks = 2 * lines
    unit = cols // blocks
    wide = feats // SPLIT

    def parts(m):
        return range(m * SPLIT, (m + 1) * SPLIT)

    def lanes_of(v):
        return slice(v % SPLIT * wide, (v % SPLIT + 1) * wide)

    me = lax.axis_index("tok")
    core, chip = lax.rem(me, 2), lax.div(me, 2)
    x, y, line = lax.rem(chip, 2), lax.rem(lax.div(chip, 2), 2), lax.div(chip, 4)
    a, b = x + core * (y - x), y + core * (x - y)
    a_other, b_other = b, a
    other = 1 - core
    partner = device(line, x, y, other)
    pair = in_role(line, 1 - a, b, core)
    side = in_role(line, a, 1 - b, core)
    pair_takes = in_role(line, 1 - a_other, b_other, other)
    mirror_line = lax.rem(line + half, lines)
    mirror = in_role(mirror_line, a, b, core)
    upper = lax.div(line, half)
    place = line - upper * half
    base = upper * half

    def mate(i):
        return in_role(base + lax.rem(place + i, half), a, b, core)

    def around(i):
        return lax.rem(me + count + i, count)

    after = around(1)
    loads = [pltpu.make_async_copy(refs[i], loaded[i], load_sem.at[i]) for i in range(8)]
    loading = (0, 1, 2, 4, 7, 5, 6, 3)
    for i in loading:
        loads[i].start()

    barrier = pltpu.get_barrier_semaphore()
    plane = line * 8
    known = [plane + lax.rem(me - plane + i, 8) for i in range(1, 8)]
    known += [mirror] + [mate(i) for i in range(1, half)]
    known += [around(i) for i in (1, -1, 8, -8)]
    for one in known:
        pl.semaphore_signal(
            barrier, inc=1, device_id={"tok": one}, device_id_type=pl.DeviceIdType.MESH
        )
    for i in loading:
        loads[i].wait()
    for group in range(FAST_HEADS):
        rsend[group] = jnp.broadcast_to(rate_ref[group : group + 1, :], (8, tokens))
    pl.semaphore_wait(barrier, len(known))

    started = []

    def go(copy):
        copy.start()
        started.append(copy)

    head = upper
    head_a, head_b = x + head * (y - x), y + head * (x - y)
    stored = place * 4 + y * 2 + x

    def first(m, far):
        cross, apart = far % 2, far // 2
        start = (head_a + cross - 2 * cross * head_a) * cols
        src = w_refs[m].at[:, pl.ds(pl.multiple_of(start, cols), cols)]
        dst = wbuf.at[m, stored, pl.ds(pl.multiple_of(core * rows, rows), rows), :]
        to_a = 1 - head_a if cross else head_a
        to = in_role(line, to_a, 1 - head_b if apart else head_b, head)
        return remote(src, dst, first_s.at[m, far], first_r.at[m, far, core], to)

    def first_here(m):
        src = w_refs[m].at[:, pl.ds(pl.multiple_of(head_a * cols, cols), cols)]
        dst = wbuf.at[m, stored, pl.ds(pl.multiple_of(core * rows, rows), rows), :]
        return pltpu.make_async_copy(src, dst, first_l.at[m])

    def reach(m):
        return 4 if m in WIDE else 2

    for m in range(3):
        for far in range(1, reach(m)):
            go(first(m, far))

        @pl.when(core == head)
        def _():
            first_here(m).start()

        @pl.when(core != head)
        def _():
            first(m, 0).start()

    def own_lanes(group):
        return pl.ds(pl.multiple_of(group * feats, feats), feats)

    def send_tokens(kind):
        ref, buf = ((k_ref, kbuf), (v_ref, vbuf), (q_ref, qbuf), (rsend, rbuf))[kind]
        if kind == 3:
            mine, theirs = ref.at[core], ref.at[other]
        else:
            mine, theirs = ref.at[:, own_lanes(core)], ref.at[:, own_lanes(other)]
        here, there = buf.at[a * 2 + core], buf.at[a_other * 2 + core]
        go(remote(mine, here, tok_s.at[kind, 0], tok_r.at[kind, 1 + core], pair))
        go(remote(theirs, there, tok_s.at[kind, 1], tok_r.at[kind, 0], partner))
        go(remote(theirs, there, tok_s.at[kind, 2], tok_r.at[kind, 1 + core], pair_takes))
        if kind == 3:
            rbuf[a * 2 + core] = rsend[core]
        else:
            buf[a * 2 + core] = ref[:, own_lanes(core)]

    def take_tokens(kind):
        buf = (kbuf, vbuf, qbuf, rbuf)[kind]
        for i, slot in ((0, a * 2 + other), (1, (1 - a) * 2), (2, (1 - a) * 2 + 1)):
            ref = buf.at[slot]
            remote(ref, ref, tok_s.at[kind, i], tok_r.at[kind, i], partner).wait_recv()

    send_tokens(0)
    send_tokens(3)
    send_tokens(1)

    def pairs(m):
        return 1 if m in WIDE else 2

    def piece(m, k, i, b_from):
        if m in WIDE:
            return wbuf.at[m, pl.ds(k * 4, 4)]
        return wbuf.at[m, k * 4 + b_from * 2 + i + core * (i - b_from)]

    def first_wait(m):
        first_here(m).wait()
        for far in range(reach(m)):
            from_a = 1 - a if far % 2 else a
            from_b = 1 - b if far // 2 else b
            block = wbuf.at[m, place * 4 + from_b * 2 + from_a + core * (from_a - from_b)]
            for c in (other,) if far == 0 else (0, 1):
                ref = block.at[pl.ds(pl.multiple_of(c * rows, rows), rows), :]
                copy = remote(ref, ref, first_s.at[m, far], first_r.at[m, far, c], partner)
                copy.wait_recv()

    def to_mirror(m, i):
        ref = piece(m, place, i, b)
        return remote(ref, ref, mirror_s.at[m, i], mirror_r.at[m, i], mirror)

    def to_mate(m, i, step):
        ref = piece(m, place, i, b)
        return remote(ref, ref, mate_s.at[m, i, step], mate_r.at[m, i, step], mate(step))

    def from_mate(m, i, step):
        ref = piece(m, lax.rem(place + half - step, half), i, b)
        return remote(ref, ref, mate_s.at[m, i, step], mate_r.at[m, i, step], mate(step))

    def to_side(m, i, step):
        ref = piece(m, lax.rem(place + half - step, half), i, b)
        return remote(ref, ref, side_s.at[m, i, step], side_r.at[m, i, step], side)

    def from_side(m, i, step):
        ref = piece(m, lax.rem(place + half - step, half), i, 1 - b)
        return remote(ref, ref, side_s.at[m, i, step], side_r.at[m, i, step], side)

    for m in range(3):

        @pl.when(core == head)
        def _():
            first_wait(m)
            for i in range(pairs(m)):
                to_mirror(m, i).start()

        @pl.when(core != head)
        def _():
            for i in range(pairs(m)):
                to_mirror(m, i).wait_recv()

        for i in range(pairs(m)):
            for step in range(1, half):
                go(to_mate(m, i, step))
            if m not in WIDE:
                go(to_side(m, i, 0))
    for m in range(3):
        if m in WIDE:
            continue
        for step in range(1, half):
            for i in range(2):
                from_mate(m, i, step).wait_recv()
                go(to_side(m, i, step))

    def weight_there(m):
        if m in WIDE:
            for step in range(1, half):
                from_mate(m, 0, step).wait_recv()
            return
        for step in range(half):
            for i in range(2):
                from_side(m, i, step).wait_recv()

    def weight(m):
        return wbuf[m].reshape(feats, cols)

    all_keys = lambda: kbuf[...].reshape(4 * tokens, feats)
    all_values = lambda: vbuf[...].reshape(4 * tokens, feats)

    def part_of(which):
        return pl.ds(pl.multiple_of(which * (cols // 2), cols // 2), cols // 2)

    def spread(s):
        column = turned(rbuf[s][0:1, :], tokens)
        return jnp.concatenate([column] * (cols // 2 // tokens), axis=1)

    def keep(m, s, which, value):
        lanes = pl.ds(pl.multiple_of(s * tokens, tokens), tokens)
        hid[m, part_of(which), lanes] = jnp.transpose(value).astype(jnp.bfloat16)

    def weigh(which):
        def one(s, carry):
            a_one, a_three = asum[ONE, s, :, part_of(which)], asum[THREE, s, :, part_of(which)]
            keep(TWO, s, which, -spread(s) * a_one * jax.nn.sigmoid(a_one) * a_three)
            return carry

        lax.fori_loop(0, 4, one, 0)

    line_bit = [bit_of(line, i) for i in range(line_bits)]
    starts = [jnp.int32(0)]
    for i in range(line_bits):
        starts.append(starts[-1] + line_bit[i] * (lines >> (i + 1)))
    pos = b * lines + starts[-1]

    def gradient(v, which):
        m = v // SPLIT
        ref = vbuf if m == TWO else kbuf
        side_rows = ref[:, :, lanes_of(v)].reshape(4 * tokens, wide)
        return dot(hid[m, part_of(which), :], side_rows).reshape(lines, unit, wide)

    def offset(step):
        return blocks - 2 * (lines >> step)

    def send_sum(m, step):
        at = pl.ds(offset(step), lines >> step)
        to = side if step == 0 else in_role(flipped(line, step - 1), a, b, core)
        return remote(
            staged.at[m, at], landed.at[m, at], sum_s.at[m, step], sum_r.at[m, step], to
        )

    def send_away(m):
        for v in parts(m):
            staged[v, pl.ds(0, lines)] = gradient(v, 1 - b).astype(jnp.bfloat16)
            go(send_sum(v, 0))

    def keep_own(m):
        for v in parts(m):
            total[v] = gradient(v, b)

    def keep_old(m):
        lanes = pl.ds(pl.multiple_of(b * (cols // 2), cols // 2), cols // 2)
        mine = wbuf[m, :, :, lanes].reshape(feats, cols // 2).astype(jnp.float32)
        old_all[...] = jnp.transpose(mine).reshape(lines, unit, feats)
        old_own[m] = old_all[starts[-1]]

    def deltas(which):
        def one(s, carry):
            a_one, a_three = asum[ONE, s, :, part_of(which)], asum[THREE, s, :, part_of(which)]
            back = -spread(s) * asum[TWO, s, :, part_of(which)]
            sig = jax.nn.sigmoid(a_one)
            keep(ONE, s, which, back * a_three * sig * (1.0 + a_one * (1.0 - sig)))
            keep(THREE, s, which, back * a_one * sig)
            return carry

        lax.fori_loop(0, 4, one, 0)

    order = (TWO, ONE, THREE)

    def pass_on(m, step):
        size = lines >> step
        bit = line_bit[step - 1]
        kept, away = starts[step], starts[step - 1] + (1 - bit) * size
        shift = offset(step - 1) - starts[step - 1]
        send_sum(m, step - 1).wait_recv()

        def stage(i, carry):
            value = total[m, away + i] + landed[m, shift + away + i].astype(jnp.float32)
            staged[m, offset(step) + i] = value.astype(jnp.bfloat16)
            return carry

        def hold(i, carry):
            value = total[m, kept + i] + landed[m, shift + kept + i].astype(jnp.float32)
            total[m, kept + i] = value
            return carry

        lax.fori_loop(0, size, stage, 0)
        go(send_sum(m, step))
        lax.fori_loop(0, size, hold, 0)

    def pass_all(m, step):
        for v in parts(m):
            pass_on(v, step)

    seg_copy = remote(seg_ref, old_seg, halo_s.at[4], halo_r.at[4], after)
    kinds = ((k_ref, kbuf, old_k), (v_ref, vbuf, old_v))

    def upward(i):
        src = kinds[i][1].at[3]
        return remote(src, relay.at[i], up_s.at[i], up_r.at[i], around(8))

    def halo(i, group, relayed=False):
        ref, buf, old = kinds[i]
        if group is None:
            return remote(ref, old, halo_s.at[i], halo_r.at[i], partner)
        at = old.at[:, pl.ds(group * feats, feats)]
        if group == 0:
            slot, to = 3, device(line, 0, 1 - y, 0)
        else:
            slot, to = (y + x - 2 * x * y) * 2 + 1, device(line, 1 - x, y, 0)
        src = relay.at[i] if relayed else buf.at[slot]
        return remote(src, at, halo_s.at[i * 2 + group], halo_r.at[i * 2 + group], to)

    def halo_from(i, group):
        if group is None:
            return halo(i, None)
        at = kinds[i][2].at[:, pl.ds(group * feats, feats)]
        return remote(at, at, halo_s.at[i * 2 + group], halo_r.at[i * 2 + group], partner)

    edge_zero = (core == 0) & (x == 0) & (y == 1)
    edge_one = (core == 1) & (x == 1) & (y == 0)
    edge = edge_zero | edge_one
    plain_zero = (core == 0) & (x == 0) & (y == 0)
    plain_one = (core == 1) & jnp.logical_not(edge_one)

    def both(predicate, act):
        @pl.when(predicate)
        def _():
            for i in range(2):
                act(i)

    def halo_sends(act):
        both(core == 0, lambda i: act(halo(i, None)))
        both(plain_zero, lambda i: act(halo(i, 0)))
        both(plain_one, lambda i: act(halo(i, 1)))
        both(edge_zero & (line > 0), lambda i: act(halo(i, 0, True)))
        both(edge_one & (line > 0), lambda i: act(halo(i, 1, True)))

        @pl.when(me != count - 1)
        def _():
            act(seg_copy)

    def project(m):
        weight_there(m)
        rows_in = all_values() if m == TWO else all_keys()
        asum[m] = dot(rows_in, weight(m)).reshape(4, tokens, cols)

    take_tokens(0)
    take_tokens(3)
    project(ONE)
    project(THREE)
    weigh(1 - b)
    take_tokens(1)
    both(edge & (line < lines - 1), lambda i: upward(i).start())
    send_away(TWO)
    weigh(b)
    keep_own(TWO)
    keep_old(ONE)
    keep_old(THREE)
    project(TWO)
    deltas(1 - b)
    send_away(ONE)
    pass_all(TWO, 1)
    send_away(THREE)
    send_tokens(2)

    both(edge & (line > 0), lambda i: upward(i).wait_recv())
    halo_sends(lambda copy: copy.start())

    @pl.when(me == 0)
    def _():
        old_k[...] = jnp.zeros_like(old_k)
        old_v[...] = jnp.zeros_like(old_v)
        old_seg[...] = jnp.zeros_like(old_seg)

    @pl.when((core == 0) & (x == 1))
    def _():
        for _, buf, old in kinds:
            old[:, 0:feats] = buf[1]

    pos_bits = line_bit[::-1] + [b]
    low = list(range(line_bits - 1))
    orders = {
        ONE: low + [line_bits - 1, line_bits],
        THREE: low + [line_bits - 1, line_bits],
        TWO: low + [PAIR, line_bits - 1, line_bits],
    }

    def moved(region, step):
        which, offs, size = region
        return (1 - which, offs, size) if step == PAIR else (which, offs ^ (1 << step), size)

    plans = {m: spread_plan(orders[m], moved) for m in order}

    def block_of(v, region):
        which, offs, size = region
        start = jnp.int32(0)
        for i, bit in enumerate(pos_bits):
            if (1 << i) >= size:
                start += (1 - bit if (offs >> i) & 1 else bit) * (1 << i)
        return new.at[v, which, pl.ds(start, size)]

    def partner_at(step):
        if step == PAIR:
            return pair
        if step == line_bits:
            return side
        return in_role(flipped(line, line_bits - 1 - step), a, b, core)

    def new_copy(v, turn, index, src, dst):
        to = partner_at(orders[v // SPLIT][turn])
        return remote(src, dst, all_s.at[v, turn, index], all_r.at[v, turn, index], to)

    def send_group(v, group):
        m = v // SPLIT
        for turn in range(group, len(orders[m])):
            for index, region in plans[m][turn]:
                if index[0] != group:
                    continue
                dst = region if orders[m][turn] != PAIR else (1 - region[0],) + region[1:]
                go(new_copy(v, turn, index[1], block_of(v, region), block_of(v, dst)))

    def new_wait(v, turn):
        m = v // SPLIT
        for index, region in plans[m][turn]:
            ref = block_of(v, moved(region, orders[m][turn]))
            new_copy(v, turn, index[1], ref, ref).wait_recv()

    def renew(m):
        updates, square = [], 0.0
        for v in parts(m):
            send_sum(v, steps - 1).wait_recv()
            grad = total[v, starts[-1]] + landed[v, offset(steps - 1)].astype(jnp.float32)
            updates.append(old_own[m, :, lanes_of(v)] - grad)
            square += jnp.sum(updates[-1] * updates[-1], axis=1, keepdims=True)
        old = old_own[m]
        old_len = jnp.sqrt(jnp.sum(old * old, axis=1, keepdims=True))
        ratio = old_len / jnp.sqrt(square + EPS)
        for v, update in zip(parts(m), updates):
            new[v, 0, pos] = (update * ratio).astype(jnp.bfloat16)
            send_group(v, 0)

    deltas(b)
    keep_own(ONE)
    pass_all(ONE, 1)
    keep_own(THREE)
    pass_all(THREE, 1)
    keep_old(TWO)
    for step in range(2, steps):
        for m in order:
            pass_all(m, step)
    for m in order:
        renew(m)

    dim = width // ATT_HEADS
    scale = 1.0 / math.sqrt(dim)

    both(core == 1, lambda i: halo_from(i, None).wait_recv())
    both((core == 0) & (x == 0) & (me != 0), lambda i: halo_from(i, 0).wait_recv())
    both((core == 0) & (me != 0), lambda i: halo_from(i, 1).wait_recv())

    @pl.when(me != 0)
    def _():
        seg_copy.wait_recv()

    def attend(first_head, last_head):
        row = lax.broadcasted_iota(jnp.int32, (tokens, tokens), 0)
        col = lax.broadcasted_iota(jnp.int32, (tokens, tokens), 1)
        seg_row = seg_ref[...].astype(jnp.float32)
        seg_col = turned(seg_row, tokens)
        now_ok = (col <= row) & (row - col < WINDOW) & (seg_col == seg_row)
        old_ok = (
            (row - col + tokens < WINDOW)
            & (seg_col == old_seg[...].astype(jnp.float32))
            & (row + me * tokens >= row + tokens)
        )

        def one(i, carry):
            lanes = pl.ds(pl.multiple_of(i * dim, dim), dim)
            q = q_ref[:, lanes]

            def score(keys, allowed):
                return jnp.where(allowed, nt_dot(q, keys) * scale, jnp.float32(-1e30))

            old, now = score(old_k[:, lanes], old_ok), score(k_ref[:, lanes], now_ok)
            top = jnp.maximum(
                jnp.max(old, axis=1, keepdims=True), jnp.max(now, axis=1, keepdims=True)
            )
            old = jnp.where(old_ok, jnp.exp(old - top), jnp.float32(0.0))
            now = jnp.where(now_ok, jnp.exp(now - top), jnp.float32(0.0))
            norm = jnp.sum(old, axis=1, keepdims=True) + jnp.sum(now, axis=1, keepdims=True)
            out = dot((old / norm).astype(jnp.bfloat16), old_v[:, lanes]) + dot(
                (now / norm).astype(jnp.bfloat16), v_ref[:, lanes]
            )
            att_ref[:, lanes] = out.astype(jnp.bfloat16)
            return carry

        lax.fori_loop(first_head, last_head, one, 0)

    def query_dot(m, rows_q):
        return sum(nt_dot(rows_q[:, lanes_of(v)], flat(new[v, 0])) for v in parts(m))

    def mixed(place_from):
        slots = pl.ds(place_from * 2, 2)
        b_one = asum[ONE, slots].reshape(2 * tokens, cols)
        b_three = query_dot(THREE, qbuf[slots].reshape(2 * tokens, feats))
        return (jax.nn.silu(b_one) * b_three).astype(jnp.bfloat16)

    turns = [
        (turn, v)
        for turn in range(steps + 1)
        for m in order
        for v in parts(m)
        if turn < len(orders[m]) and turn < steps
    ]
    slots = len(turns) - 2
    for slot, (turn, v) in enumerate(turns):
        new_wait(v, turn)
        send_group(v, turn + 1)
        if slot < slots:
            attend(ATT_HEADS * slot // slots, ATT_HEADS * (slot + 1) // slots)
        if (turn, v) == (steps - 1, parts(ONE)[-1]):
            take_tokens(2)
            rows_q = qbuf[...].reshape(4 * tokens, feats)
            asum[ONE] = query_dot(ONE, rows_q).reshape(4, tokens, cols)

    z_send[...] = mixed(1 - a)
    z_copy = remote(z_send, z_peer, end_s.at[0], end_r.at[0], pair)
    go(z_copy)
    z_own[...] = mixed(a)
    for v in parts(TWO):
        new_wait(v, steps)
    z_copy.wait_recv()

    def fast_rows(c, v):
        at = pl.ds(pl.multiple_of(c * tokens, tokens), tokens)
        value = dot(z_own[at, :], flat(new[v, 0])) + dot(z_peer[at, :], flat(new[v, 1]))
        return value.astype(jnp.bfloat16)

    def out_copy(v, group):
        lanes = pl.ds(pl.multiple_of(group * feats + v % SPLIT * wide, wide), wide)
        src, at = o_send.at[:, pl.ds(v % SPLIT * wide, wide)], 1 + v % SPLIT
        return remote(src, out_ref.at[:, lanes], end_s.at[at], end_r.at[at], partner)

    for v in parts(TWO):
        o_send[:, lanes_of(v)] = fast_rows(other, v)
        go(out_copy(v, core))
    for v in parts(TWO):
        lanes = pl.ds(pl.multiple_of(core * feats + v % SPLIT * wide, wide), wide)
        out_ref[:, lanes] = fast_rows(core, v)
    for v in parts(TWO):
        out_copy(v, other).wait_recv()

    for copy in started:
        copy.wait_send()
    for m in range(3):

        @pl.when(core == head)
        def _():
            for i in range(pairs(m)):
                to_mirror(m, i).wait_send()

        @pl.when(core != head)
        def _():
            first(m, 0).wait_send()

    halo_sends(lambda copy: copy.wait_send())
    both(edge & (line < lines - 1), lambda i: upward(i).wait_send())


def per_device(queries, keys, values, segment, rates, fast_one, fast_three, fast_two):
    count = lax.axis_size("tok")
    tokens, width = queries.shape
    rows, hidden = fast_one.shape
    lines = count // 8
    half = lines // 2
    steps = lines.bit_length()
    feats = width // FAST_HEADS
    cols = hidden // 2
    blocks = 2 * lines
    unit = cols // blocks
    wide = feats // SPLIT
    bf16, f32 = jnp.bfloat16, jnp.float32
    dma = pltpu.SemaphoreType.DMA
    operands = (
        fast_one, fast_three, fast_two, queries, keys, values, segment.reshape(1, tokens), rates.T
    )
    return pl.pallas_call(
        functools.partial(kernel, count),
        out_shape=[jax.ShapeDtypeStruct(queries.shape, bf16)] * 2,
        in_specs=[pl.BlockSpec(memory_space=pltpu.HBM)] * 8,
        out_specs=[pl.BlockSpec(memory_space=pltpu.VMEM)] * 2,
        scratch_shapes=[pltpu.VMEM(one.shape, one.dtype) for one in operands]
        + [
            dma((8,)),
            pltpu.VMEM((3, count // 4, 2 * rows, cols), bf16),
            pltpu.VMEM((4, tokens, feats), bf16),
            pltpu.VMEM((4, tokens, feats), bf16),
            pltpu.VMEM((4, tokens, feats), bf16),
            pltpu.VMEM((4, 8, tokens), f32),
            pltpu.VMEM((FAST_HEADS, 8, tokens), f32),
            pltpu.VMEM((3, 4, tokens, cols), f32),
            pltpu.VMEM((3, cols, 4 * tokens), bf16),
            pltpu.VMEM((3 * SPLIT, lines, unit, wide), f32),
            pltpu.VMEM((3 * SPLIT, blocks, unit, wide), bf16),
            pltpu.VMEM((3 * SPLIT, blocks, unit, wide), bf16),
            pltpu.VMEM((3, unit, feats), f32),
            pltpu.VMEM((lines, unit, feats), f32),
            pltpu.VMEM((3 * SPLIT, 2, blocks, unit, wide), bf16),
            pltpu.VMEM((2 * tokens, cols), bf16),
            pltpu.VMEM((2 * tokens, cols), bf16),
            pltpu.VMEM((2 * tokens, cols), bf16),
            pltpu.VMEM((tokens, feats), bf16),
            pltpu.VMEM(keys.shape, bf16),
            pltpu.VMEM(values.shape, bf16),
            pltpu.VMEM((1, tokens), jnp.int32),
            pltpu.VMEM((2, tokens, feats), bf16),
            dma((3, 4)),
            dma((3, 4, 2)),
            dma((3,)),
            dma((3, 2)),
            dma((3, 2)),
            dma((3, 2, half)),
            dma((3, 2, half)),
            dma((3, 2, half)),
            dma((3, 2, half)),
            dma((4, 3)),
            dma((4, 3)),
            dma((3 * SPLIT, steps)),
            dma((3 * SPLIT, steps)),
            dma((3 * SPLIT, steps + 1, 2 * steps)),
            dma((3 * SPLIT, steps + 1, 2 * steps)),
            dma((1 + SPLIT,)),
            dma((1 + SPLIT,)),
            dma((5,)),
            dma((5,)),
            dma((2,)),
            dma((2,)),
        ],
        compiler_params=pltpu.CompilerParams(
            collective_id=0, has_side_effects=True, vmem_limit_bytes=40 << 20
        ),
    )(*[pltpu.with_memory_space_constraint(one, pltpu.HBM) for one in operands])


def solution(mesh):
    placed = P(("grp", "tok"), None)
    return jax.shard_map(
        per_device,
        mesh=mesh,
        in_specs=(placed, placed, placed, P(("grp", "tok")), placed, placed, placed, placed),
        out_specs=(placed, placed),
        check_vma=False,
    )
```
